32 devices in a mesh: rep: 1 (over z), r: 4 (over y), s: 8 (over x, core).
Axes of the slice: x: 4, y: 4, z: 1, core: 2. Of those that a mesh axis runs over, the one named last changes fastest.
The devices are a block of a 4x4x8 slice.
Arguments:
- x: bfloat16 [32, 2048, 1024], P(('rep', 'r', 's'))
- dy: bfloat16 [32, 2048, 1024], P(('rep', 'r', 's'))
- w_gate: bfloat16 [2, 1024, 3584], P(None, 's')
- w_up: bfloat16 [2, 1024, 3584], P(None, 's')
- w_down: bfloat16 [2, 3584, 1024], P(None, 's')
Outputs:
- output 1: bfloat16 [32, 2048, 1024], P(('rep', 'r', 's'))
- output 2: bfloat16 [2, 1024, 3584], P('rep', 's')
- output 3: bfloat16 [2, 1024, 3584], P('rep', 's')
- output 4: bfloat16 [2, 3584, 1024], P('rep', 's')
All inputs are finite; a program needn't handle non-finite values.
Results may differ from the reference program's by a relative error of at most 0.018.
Values are sent between devices in bfloat16 or wider.
A program may use at most 768 MiB of HBM per device.

```python
import jax
import jax.numpy as jnp
from jax import lax

SEQUENCES = 32
TOKENS = 2048
D = 1024
FF = 3584
LAYERS = 2
NAMES = ("w_gate", "w_up", "w_down")
SHAPES = {"w_gate": (LAYERS, D, FF), "w_up": (LAYERS, D, FF), "w_down": (LAYERS, FF, D)}


def bump(key, n, height):
    away = (jnp.arange(n, dtype=jnp.int32) - jax.random.randint(key, (), 0, n, jnp.int32)) % n
    return jnp.where(away < n // 8, height, 1.0)


def together(key, own, strength):
    shared = jax.random.normal(key, own.shape[1:], jnp.float32)
    return (own + strength * shared) * lax.rsqrt(1 + strength * strength)


def setup_inputs(seed: int = 0, part: int = 0) -> dict:
    kx, kdy, ka, kb, kz, kf, kh, kl, *kw = jax.random.split(jax.random.key(seed), 8 + len(NAMES))
    kx, kdy, ka, kb = (jax.random.fold_in(k, part) for k in (kx, kdy, ka, kb))
    shape = (SEQUENCES, TOKENS, D)
    much_x, much_dy = jax.random.uniform(kz, (2,), jnp.float32, 0.0, 1.0)
    layers = 2.0 ** jax.random.uniform(kl, (LAYERS, 1, 1), jnp.float32, -1.0, 1.0)
    x = together(ka, jax.random.normal(kx, shape, jnp.float32), much_x) * bump(kf, D, 4.0)
    dy = together(kb, jax.random.normal(kdy, shape, jnp.float32), much_dy)
    drawn = {"x": x.astype(jnp.bfloat16), "dy": (dy * (SEQUENCES * TOKENS) ** -0.5).astype(jnp.bfloat16)}
    for key, name in zip(kw, NAMES, strict=True):
        w = jax.random.normal(key, SHAPES[name], jnp.float32) * SHAPES[name][1] ** -0.5
        drawn[name] = (w * {"w_gate": 1.0, "w_up": bump(kh, FF, 4.0), "w_down": layers}[name]).astype(jnp.bfloat16)
    return drawn


def matmul(a, w):
    return jnp.dot(a, w, preferred_element_type=jnp.float32).astype(jnp.bfloat16)


def normed(h):
    wide = h.astype(jnp.float32)
    scale = lax.rsqrt(jnp.mean(wide**2, -1, keepdims=True) + 1e-6)
    return (wide * scale).astype(jnp.bfloat16)


def layer(h, w):
    a = normed(h)
    gate = jnp.dot(a, w["w_gate"], preferred_element_type=jnp.float32)
    up = jnp.dot(a, w["w_up"], preferred_element_type=jnp.float32)
    return h + matmul((jax.nn.silu(gate) * up).astype(jnp.bfloat16), w["w_down"])


def stack(weights, h):
    return lax.scan(lambda h, w: (layer(h, w), None), h, weights)[0]


def reference(x, dy, w_gate, w_up, w_down):
    weights = dict(zip(NAMES, (w_gate, w_up, w_down), strict=True))

    def take(so_far, sequence):
        h, by_y = sequence
        _, back = jax.vjp(stack, weights, h)
        by_weights, by_h = back(by_y)
        return jax.tree.map(lambda total, term: total + term.astype(jnp.float32), so_far, by_weights), by_h

    none_yet = {name: jnp.zeros(w.shape, jnp.float32) for name, w in weights.items()}
    by_weights, by_x = lax.scan(take, none_yet, (x, dy))
    return (by_x, *(by_weights[name].astype(jnp.bfloat16) for name in NAMES))
```

```python
import functools

import jax
import jax.numpy as jnp
from jax import lax
from jax.experimental import pallas as pl
from jax.experimental.pallas import tpu as pltpu
from jax.sharding import PartitionSpec as P

BF, F32 = jnp.bfloat16, jnp.float32
MESH = pl.DeviceIdType.MESH
CORES = 2
BW = 128
TILES = 4
G_, U_, D_ = 0, 1, 2


def dot(a, b, ca=1, cb=0):
    return lax.dot_general(a, b, (((ca,), (cb,)), ((), ())), preferred_element_type=F32)


def when(condition, f):
    if isinstance(condition, bool):
        if condition:
            f()
    else:
        pl.when(condition)(f)


def kernel(dims, x_ref, dy_ref, own,
           by_x, og, od, G, ST, PT, A0T, H1,
           a_nat, a_t, dyv, acc, wbuf, dgu, pt, stb,
           s_send, d_recv, own32, r32, l32, s_u1, s_pr, s_pl, u2r, u2l, ra, rb, rc, rd, v, ya, yb, yc, f_out,
           g_send, g_recv, w_sem, st_sem, pt_sem, ld_sem, rs_send, d_sem, x_sem, rc_sem, y_sem, o_sem, od_send, od_recv):
    nx, ny, C, T, D = dims
    TM = T // TILES
    N = 2 * C
    DR = D // (CORES * nx)
    HR, QR = DR // 2, DR // 4
    CW = nx * BW
    DH = D // 2

    s, y = lax.axis_index("s"), lax.axis_index("r")
    X, k = lax.div(s, CORES), lax.rem(s, CORES)
    at = lambda xx, kk: CORES * lax.rem(xx, nx) + kk
    right, left = {"s": at(X + 1, k)}, {"s": at(X + nx - 1, k)}
    sib = {"s": at(X, 1 - k)}
    up, down = {"r": lax.rem(y + 1, ny)}, {"r": lax.rem(y + ny - 1, ny)}

    barrier = pltpu.get_barrier_semaphore()
    for who in (right, left, sib, up, down):
        pl.semaphore_signal(barrier, inc=1, device_id=who, device_id_type=MESH)
    pl.semaphore_wait(barrier, 5)

    def remote(src, dst, ss, rs, who):
        return pltpu.make_async_remote_copy(src_ref=src, dst_ref=dst, send_sem=ss, recv_sem=rs, device_id=who, device_id_type=MESH)

    def arrived(dst, rs):
        pltpu.make_async_copy(dst, dst, rs).wait()

    pL, pR, pO = at(X + nx - 1, k), at(X + 1, k), at(X + 2, k)
    par = lax.rem(y, 2)
    mine, other = par * HR, (1 - par) * HR

    def rows(base, q):
        return pl.ds(pl.multiple_of(base + q * QR, QR), QR)

    def out_copy(t, n):
        full = pl.ds(0, DR)
        spec = {
            0: (None, rows(mine, 0), right), 1: (None, rows(mine, 1), right),
            2: (None, rows(mine, 1), left), 3: (None, rows(mine, 0), left),
            4: (pL, rows(mine, 0), right), 5: (pR, rows(mine, 1), left),
            6: (pL, rows(mine, 0), up), 7: (pR, rows(mine, 0), up), 8: (pO, rows(mine, 0), up),
            9: (pL, rows(mine, 1), down), 10: (pR, rows(mine, 1), down), 11: (pO, rows(mine, 1), down),
            12: (None, full, sib), 13: (pL, full, sib), 14: (pR, full, sib), 15: (pO, full, sib),
        }
        j, r, who = spec[t]
        src = own.at[n, :, r, :] if j is None else G.at[n, :, j, r, :]
        return remote(src, G.at[n, :, s if j is None else j, r, :], g_send.at[n, t], g_recv.at[n, t], who)

    def in_wait(t, n):
        full = pl.ds(0, DR)
        oL, oR, oO, oS = at(X + nx - 1, 1 - k), at(X + 1, 1 - k), at(X + 2, 1 - k), at(X, 1 - k)
        spec = {
            0: (pL, rows(mine, 0)), 1: (pL, rows(mine, 1)), 2: (pR, rows(mine, 1)), 3: (pR, rows(mine, 0)),
            4: (pO, rows(mine, 0)), 5: (pO, rows(mine, 1)),
            6: (pL, rows(other, 0)), 7: (pR, rows(other, 0)), 8: (pO, rows(other, 0)),
            9: (pL, rows(other, 1)), 10: (pR, rows(other, 1)), 11: (pO, rows(other, 1)),
            12: (oS, full), 13: (oL, full), 14: (oR, full), 15: (oO, full),
        }
        j, r = spec[t]
        arrived(G.at[n, :, j, r, :], g_recv.at[n, t])

    def stage(f):
        def run(n):
            when((n >= 0) & (n < N) if not isinstance(n, int) else 0 <= n < N, lambda: f(n))
        return run

    def starts(n, *ts):
        for t in ts:
            out_copy(t, n).start()

    @stage
    def gA(n):
        starts(n, 0, 2, 1, 3, 12)

    @stage
    def gB(n):
        in_wait(0, n)
        starts(n, 4, 6)
        in_wait(2, n)
        starts(n, 5, 10)

    @stage
    def gC(n):
        in_wait(1, n)
        starts(n, 9)
        in_wait(3, n)
        starts(n, 7)

    @stage
    def gD(n):
        in_wait(4, n)
        starts(n, 8)
        in_wait(5, n)
        starts(n, 11)

    @stage
    def gE(n):
        for a, b, t in ((6, 9, 13), (7, 10, 14), (8, 11, 15)):
            in_wait(a, n)
            in_wait(b, n)
            starts(n, t)

    def load_weights(n, slot):
        pltpu.make_async_copy(own.at[n], wbuf.at[slot, :, s], w_sem.at[slot]).start()
        for j in range(1, CORES * nx):
            p = lax.rem(s + j, CORES * nx)
            pltpu.make_async_copy(G.at[n, :, p], wbuf.at[slot, :, p], w_sem.at[slot]).start()

    def wait_weights(slot):
        pltpu.make_async_copy(wbuf.at[slot], wbuf.at[slot], w_sem.at[slot]).wait()

    @stage
    def gF(n):
        for t in (12, 13, 14, 15):
            in_wait(t, n)
        load_weights(n, lax.rem(n, 2))

    def w_cols(slot, q):
        return wbuf[slot, q].reshape(D, CW)

    def w_half(slot, q, h):
        return wbuf[slot, q, pl.ds(h * nx, nx)].reshape(DH, CW)

    def wd_half(slot, h):
        return jnp.concatenate([wbuf[slot, D_, CORES * j + h] for j in range(nx)], axis=0)

    def tile(i, n=None):
        n = TM if n is None else n
        return pl.ds(pl.multiple_of(i * n, n), n)

    def rel(j):
        return lax.rem(X + j, nx)

    def lane_lhs(lane):
        return jnp.concatenate([a_t[rel(j), lane] for j in range(nx)], axis=0)

    def grad(q, lane):
        if q == D_:
            lhs = jnp.concatenate([pt[rel(j)] for j in range(nx)], axis=0)
            return dot(lhs, dyv[lane])
        return dot(lane_lhs(lane), dgu[q])

    def d_copy(q, m):
        return remote(s_send.at[q], d_recv.at[lax.rem(m, 2), q], rs_send.at[q], d_sem.at[lax.rem(m, 2), q], sib)

    def send_lane(q, m):
        when(m > 0, lambda: d_copy(q, m).wait_send())
        s_send[q] = grad(q, 1 - k).astype(BF).reshape(nx, DR, CW)
        d_copy(q, m).start()

    lo, hi = pl.ds(0, HR), pl.ds(HR, HR)

    def x_copy(t, m):
        two, three = lax.rem(m, 2), lax.rem(m, 3)
        src, dst, sem, who = {
            0: (s_u1.at[:, lo], ra.at[two], x_sem.at[two, 0], right),
            1: (s_u1.at[:, hi], rb.at[two], x_sem.at[two, 1], left),
            2: (s_pr, rc.at[three, :, hi], rc_sem.at[three, 0], right),
            3: (s_pl, rd.at[three, :, lo], rc_sem.at[three, 1], left),
            4: (u2r, rc.at[three, :, lo], rc_sem.at[three, 2], right),
            5: (u2l, rd.at[three, :, hi], rc_sem.at[three, 3], left),
        }[t]
        return remote(src, dst, rs_send.at[3 + t], sem, who)

    def x_wait(t, m):
        two, three = lax.rem(m, 2), lax.rem(m, 3)
        dst, sem = {
            0: (ra.at[two], x_sem.at[two, 0]),
            1: (rb.at[two], x_sem.at[two, 1]),
            2: (rc.at[three, :, hi], rc_sem.at[three, 0]),
            3: (rd.at[three, :, lo], rc_sem.at[three, 1]),
            4: (rc.at[three, :, lo], rc_sem.at[three, 2]),
            5: (rd.at[three, :, hi], rc_sem.at[three, 3]),
        }[t]
        arrived(dst, sem)

    def y_copy(t, m):
        three = lax.rem(m, 3)
        src, dst, who = {
            0: (v.at[three, :, lo], ya.at[three, :, lo], up),
            1: (v.at[three, :, hi], ya.at[three, :, hi], up),
            2: (v.at[three, :, hi], yb.at[three, :, hi], down),
            3: (v.at[three, :, lo], yb.at[three, :, lo], down),
            4: (ya.at[three, :, lo], yc.at[three, :, lo], up),
            5: (yb.at[three, :, hi], yc.at[three, :, hi], down),
        }[t]
        return remote(src, dst, y_sem.at[0, three, t], y_sem.at[1, three, t], who)

    def y_wait(t, m):
        three = lax.rem(m, 3)
        dst = {0: ya.at[three, :, lo], 1: ya.at[three, :, hi], 2: yb.at[three, :, hi], 3: yb.at[three, :, lo],
               4: yc.at[three, :, lo], 5: yc.at[three, :, hi]}[t]
        arrived(dst, y_sem.at[1, three, t])

    def keep_lane(q, m):
        two = lax.rem(m, 2)
        arrived(d_recv.at[two, q], d_sem.at[two, q])
        total = (grad(q, k) + d_recv[two, q].reshape(CW, CW).astype(F32)).reshape(nx, DR, CW)
        own32[two, q] = total[0]
        r32[q] = total[1, :HR]
        s_pr[q] = total[1, HR:].astype(BF)
        s_u1[q] = total[2].astype(BF)
        s_pl[q] = total[3, :HR].astype(BF)
        l32[q] = total[3, HR:]

    def before_keep(m):
        def f():
            for t in range(4):
                x_copy(t, m - 1).wait_send()
        when(m > 0, f)

    def x1(m):
        for t in range(4):
            x_copy(t, m).start()

    def x2(m):
        x_wait(0, m)
        x_wait(1, m)

        def f():
            x_copy(4, m - 1).wait_send()
            x_copy(5, m - 1).wait_send()
        when(m > 0, f)
        two = lax.rem(m, 2)
        for q in range(3):
            u2r[q] = (r32[q] + ra[two, q].astype(F32)).astype(BF)
            u2l[q] = (l32[q] + rb[two, q].astype(F32)).astype(BF)
        x_copy(4, m).start()
        x_copy(5, m).start()

    def x3(m):
        for t in (2, 3, 4, 5):
            x_wait(t, m)
        two, three = lax.rem(m, 2), lax.rem(m, 3)
        for q in range(3):
            v[three, q] = (own32[two, q] + rc[three, q].astype(F32) + rd[three, q].astype(F32)).astype(BF)
        for t in range(4):
            y_copy(t, m).start()

    def y2(m):
        y_wait(0, m)
        y_copy(4, m).start()
        y_wait(2, m)
        y_copy(5, m).start()

    def where_m(m):
        first = m < C
        return jnp.where(first, 1, 0), jnp.where(first, m, m - C)

    def od_place(h):
        o = jnp.where(h >= C, 1, 0)
        return o, pl.ds(pl.multiple_of(HR * (h - C * o), HR), HR)

    def od_cols():
        return pl.ds(pl.multiple_of(k * DH, DH), DH)

    def og_copy(q, m):
        layer, c = where_m(m)
        return pltpu.make_async_copy(f_out.at[q], og.at[layer * C + c, q], o_sem.at[q])

    def od_each(m, local, far):
        layer, c = where_m(m)
        for e in range(2):
            o, r = od_place(2 * c + e)
            src, dst = f_out.at[D_, pl.ds(e * HR, HR)], od.at[layer, r, od_cols()]
            pl.when(o == k)(functools.partial(local, pltpu.make_async_copy(src, dst, o_sem.at[2 + e])))
            pl.when(o != k)(functools.partial(far, remote(src, dst, od_send.at[e], od_recv, sib)))

    def out_done(m):
        for q in (G_, U_):
            og_copy(q, m).wait()
        od_each(m, lambda c: c.wait(), lambda c: c.wait_send())

    def y3(m):
        for t in (1, 3, 4, 5):
            y_wait(t, m)
        when(m > 0, lambda: out_done(m - 1))
        three = lax.rem(m, 3)
        for q in range(3):
            a = v[three, q].astype(F32) + yc[three, q].astype(F32)
            b = ya[three, q].astype(F32) + yb[three, q].astype(F32)
            f_out[q] = (a + b).astype(BF)
        for t in range(6):
            y_copy(t, m).wait_send()
        for q in (G_, U_):
            og_copy(q, m).start()
        od_each(m, lambda c: c.start(), lambda c: c.start())

    def lagged(f, m):
        when(m >= 0, lambda: f(m))

    def halves(src, dst, r, sem):
        return [pltpu.make_async_copy(src.at[r, pl.ds(h * DH, DH)], dst.at[h, r], sem) for h in range(2)]

    every = pl.ds(0, T)
    for c_ in halves(x_ref.at[0], dyv, every, ld_sem.at[0]):
        c_.start()
    gA(0)
    pltpu.make_async_copy(dyv, dyv, ld_sem.at[0]).wait()

    NT = 2 * TILES
    TN = T // NT

    def both(ref, r):
        return jnp.concatenate([ref[0, r, :], ref[1, r, :]], axis=1)

    def put_a(h, i):
        r = tile(i, TN)
        scale = lax.rsqrt(jnp.mean(h * h, -1, keepdims=True) + 1e-6)
        a = (h * scale).astype(BF)
        a_nat[r, :] = a
        a_t[:, :, :, r] = a.T.reshape(nx, CORES, DR, TN)

    def norm0(i, _):
        r = tile(i, TN)
        put_a(both(dyv, r).astype(F32), i)
        acc[r, :] = jnp.zeros((TN, D), F32)
        return _

    lax.fori_loop(0, NT, norm0, 0)
    a0t_out = pltpu.make_async_copy(a_t, A0T, ld_sem.at[1])
    a0t_out.start()
    gB(0)
    gA(1)
    gC(0)
    gD(0)
    gB(1)
    gA(2)
    gC(1)
    gE(0)
    gD(1)
    gF(0)
    gB(2)
    gA(3)
    gC(2)
    gE(1)
    gD(2)

    def st_out(tau):
        return pltpu.make_async_copy(stb.at[lax.rem(tau, 2)], ST.at[tau], st_sem.at[lax.rem(tau, 2)])

    def pt_out(c, i):
        cols = tile(i)
        return pltpu.make_async_copy(pt.at[:, :, cols], PT.at[c, :, :, cols], pt_sem.at[i])

    def gate_up(slot, r):
        a = a_nat[r, :]
        g, u = dot(a, w_cols(slot, G_)), dot(a, w_cols(slot, U_))
        sig = jax.nn.sigmoid(g)
        silu = g * sig
        return silu, u * (sig + silu * (1.0 - sig)), (silu * u).astype(BF)

    def put_pt(p, i):
        pt[:, :, tile(i)] = p.T.reshape(nx, BW, TM)

    def fwd(c, carry):
        slot = lax.rem(c, 2)
        wait_weights(slot)

        def one(i, _):
            @pl.when(i == 0)
            def _0():
                gF(c + 1)
                gB(c + 3)

            @pl.when(i == 1)
            def _1():
                gA(c + 4)
                gC(c + 3)

            @pl.when(i == 2)
            def _2():
                gE(c + 2)

            @pl.when(i == 3)
            def _3():
                gD(c + 3)

            tau = TILES * c + i
            pl.when(tau >= 2)(lambda: st_out(tau - 2).wait())
            pl.when(c >= 1)(lambda: pt_out(c - 1, i).wait())
            r = tile(i)
            silu, slope, p = gate_up(slot, r)
            sb = lax.rem(tau, 2)
            stb[sb, 0] = silu
            stb[sb, 1] = slope
            put_pt(p, i)
            st_out(tau).start()
            pt_out(c, i).start()
            for h in range(2):
                acc[r, h * DH:(h + 1) * DH] += dot(p, wd_half(slot, h))
            return _

        return lax.fori_loop(0, TILES, one, carry)

    lax.fori_loop(0, C, fwd, 0)
    a0t_out.wait()
    for tau in (TILES * C - 2, TILES * C - 1):
        st_out(tau).wait()
    for i in range(TILES):
        pt_out(C - 1, i).wait()

    def h1_out(i, h):
        r = tile(i, TN)
        return pltpu.make_async_copy(dgu.at[h, r], H1.at[h, r], ld_sem.at[2])

    def norm1(i, _):
        r = tile(i, TN)
        h = (both(dyv, r).astype(F32) + acc[r, :].astype(BF).astype(F32)).astype(BF)
        for e in range(2):
            dgu[e, r, :] = h[:, e * DH:(e + 1) * DH]
            h1_out(i, e).start()
        for c_ in halves(dy_ref.at[0], dyv, r, ld_sem.at[0]):
            c_.start()
        put_a(h.astype(F32), i)
        acc[r, :] = jnp.zeros((TN, D), F32)
        return _

    lax.fori_loop(0, NT, norm1, 0)
    pltpu.make_async_copy(dgu, H1, ld_sem.at[2]).wait()
    pltpu.make_async_copy(dyv, dyv, ld_sem.at[0]).wait()

    def weights_grads(m, slot, after_p, after_keep):
        send_lane(D_, m)
        lagged(x2, m - 1)
        lagged(y2, m - 2)
        send_lane(G_, m)
        send_lane(U_, m)
        before_keep(m)
        keep_lane(D_, m)
        after_p()
        keep_lane(G_, m)
        keep_lane(U_, m)
        x1(m)
        after_keep()

        def one(i, _):
            pl.when((i == 1) & (m >= 1))(lambda: x3(m - 1))
            r = tile(i)
            for h in range(2):
                acc[r, h * DH:(h + 1) * DH] += (
                    dot(dgu[G_, r, :], w_half(slot, G_, h), 1, 1) + dot(dgu[U_, r, :], w_half(slot, U_, h), 1, 1))
            return _

        lax.fori_loop(0, TILES, one, 0)

    def d_p(slot, r):
        return dot(dyv[0, r, :], wd_half(slot, 0), 1, 1) + dot(dyv[1, r, :], wd_half(slot, 1), 1, 1)

    def put_d(r, dp, silu, slope):
        dgu[G_, r, :] = (dp * slope).astype(BF)
        dgu[U_, r, :] = (dp * silu).astype(BF)

    h1_in = [pltpu.make_async_copy(H1.at[h], a_nat.at[:, pl.ds(h * DH, DH)], ld_sem.at[0]) for h in range(2)]
    a0t_in = pltpu.make_async_copy(A0T, a_t, ld_sem.at[1])
    x_in = pltpu.make_async_copy(x_ref.at[0], a_nat, ld_sem.at[2])

    def bwd1(c, carry):
        n = C + c
        slot = lax.rem(n, 2)
        wait_weights(slot)

        def one(i, _):
            @pl.when(i == 0)
            def _0():
                gB(n + 3)

            @pl.when(i == 1)
            def _1():
                gA(n + 4)
                gC(n + 3)
                lagged(y3, c - 3)

            @pl.when(i == 2)
            def _2():
                gE(n + 2)

            @pl.when(i == 3)
            def _3():
                gD(n + 3)

            r = tile(i)
            silu, slope, p = gate_up(slot, r)
            put_pt(p, i)
            put_d(r, d_p(slot, r), silu, slope)
            return _

        lax.fori_loop(0, TILES, one, carry)
        gF(n + 1)
        last = c == C - 1

        @pl.when(last)
        def _():
            for c_ in h1_in:
                c_.start()

        weights_grads(c, slot, lambda: None, lambda: pl.when(last)(a0t_in.start))
        return carry

    lax.fori_loop(0, C, bwd1, 0)

    def st_in(tau):
        return pltpu.make_async_copy(ST.at[tau], stb.at[lax.rem(tau, 2)], st_sem.at[lax.rem(tau, 2)])

    def pt_in(c):
        return pltpu.make_async_copy(PT.at[c], pt, pt_sem.at[0])

    load_weights(0, 0)
    st_in(0).start()
    pt_in(0).start()
    pltpu.make_async_copy(a_nat, a_nat, ld_sem.at[0]).wait()

    def norm_back(h, d, through):
        scale = lax.rsqrt(jnp.mean(h * h, -1, keepdims=True) + 1e-6)
        along = jnp.sum(d * h, -1, keepdims=True) * (scale * scale * scale) * (1.0 / D)
        return (through + (d * scale - h * along)).astype(BF)

    def mid(i, _):
        r = tile(i, TN)
        out = norm_back(a_nat[r, :].astype(F32), acc[r, :], both(dyv, r).astype(F32))
        for e in range(2):
            dyv[e, r, :] = out[:, e * DH:(e + 1) * DH]
        acc[r, :] = jnp.zeros((TN, D), F32)
        return _

    lax.fori_loop(0, NT, mid, 0)
    x_in.start()
    a0t_in.wait()

    def bwd0(c, carry):
        m = C + c
        slot = lax.rem(c, 2)
        wait_weights(slot)
        pl.when(c < C - 1)(lambda: load_weights(c + 1, lax.rem(c + 1, 2)))

        def one(i, _):
            tau = TILES * c + i
            pl.when(i == 1)(lambda: y3(m - 3))
            st_in(tau).wait()
            pl.when(tau < TILES * C - 1)(lambda: st_in(tau + 1).start())
            sb = lax.rem(tau, 2)
            r = tile(i)
            put_d(r, d_p(slot, r), stb[sb, 0], stb[sb, 1])
            return _

        lax.fori_loop(0, TILES, one, carry)
        pt_in(c).wait()
        weights_grads(m, slot, lambda: pl.when(c < C - 1)(lambda: pt_in(c + 1).start()), lambda: None)
        return carry

    lax.fori_loop(0, C, bwd0, 0)

    x_in.wait()
    M = 2 * C
    x2(M - 1)
    y2(M - 2)

    def by_out(i):
        r = tile(i, TN)
        return pltpu.make_async_copy(a_nat.at[r], by_x.at[0, r], ld_sem.at[0])

    def last_norm(i, _):
        r = tile(i, TN)
        a_nat[r, :] = norm_back(a_nat[r, :].astype(F32), acc[r, :], both(dyv, r).astype(F32))
        by_out(i).start()
        return _

    lax.fori_loop(0, NT, last_norm, 0)
    x3(M - 1)
    y3(M - 3)
    y3(M - 2)
    y2(M - 1)
    y3(M - 1)
    pltpu.make_async_copy(a_nat, by_x.at[0], ld_sem.at[0]).wait()
    out_done(M - 1)
    for q in range(3):
        d_copy(q, M - 1).wait_send()
    for t in range(6):
        x_copy(t, M - 1).wait_send()
    arrived(od.at[:, :, pl.ds(0, DH)], od_recv)

    def sent(n, _):
        for t in range(16):
            out_copy(t, n).wait_send()
        return _

    lax.fori_loop(0, N, sent, 0)


def solution(mesh):
    nx, ny = mesh.shape["s"] // CORES, mesh.shape["r"]

    def step(x, dy, w_gate, w_up, w_down):
        layers, dr, ff = w_gate.shape
        _, T, D = x.shape
        C = ff // (nx * BW)
        N, CW, DH, HR = layers * C, nx * BW, D // 2, dr // 2
        TM, TN = T // TILES, T // (2 * TILES)

        k = lax.rem(lax.axis_index("s"), CORES)
        cols = lambda w: w.reshape(layers, dr, nx, C, BW).transpose(0, 3, 1, 2, 4).reshape(N, dr, CW)
        give = lax.dynamic_slice_in_dim(w_down, (1 - k) * DH, DH, 2)
        stay = lax.dynamic_slice_in_dim(w_down, k * DH, DH, 2)
        pairs = [(i, i + 1 - 2 * (i % CORES)) for i in range(mesh.shape["s"])]
        got = lax.ppermute(give, "s", pairs)
        lane = jnp.where(k == 0, jnp.concatenate([stay, got], 1), jnp.concatenate([got, stay], 1))
        own = jnp.stack([cols(w_gate), cols(w_up), lane.reshape(N, BW, DH)], 1)

        hbm = pl.BlockSpec(memory_space=pltpu.HBM)
        shape = jax.ShapeDtypeStruct
        outs = pl.pallas_call(
            functools.partial(kernel, (nx, ny, C, T, D)),
            out_shape=[
                shape((1, T, D), BF), shape((N, 2, dr, CW), BF), shape((layers, w_down.shape[1], D), BF),
                shape((N, 3, CORES * nx, dr, CW), BF), shape((TILES * C, 2, TM, CW), F32), shape((C, nx, BW, T), BF),
                shape((nx, CORES, dr, T), BF), shape((2, T, DH), BF),
            ],
            in_specs=[hbm] * 3,
            out_specs=[hbm] * 8,
            scratch_shapes=[
                pltpu.VMEM((T, D), BF), pltpu.VMEM((nx, CORES, dr, T), BF), pltpu.VMEM((2, T, DH), BF), pltpu.VMEM((T, D), F32),
                pltpu.VMEM((2, 3, CORES * nx, dr, CW), BF), pltpu.VMEM((2, T, CW), BF), pltpu.VMEM((nx, BW, T), BF),
                pltpu.VMEM((2, 2, TM, CW), F32),
                pltpu.VMEM((3, nx, dr, CW), BF), pltpu.VMEM((2, 3, nx, dr, CW), BF), pltpu.VMEM((2, 3, dr, CW), F32),
                pltpu.VMEM((3, HR, CW), F32), pltpu.VMEM((3, HR, CW), F32), pltpu.VMEM((3, dr, CW), BF),
                pltpu.VMEM((3, HR, CW), BF), pltpu.VMEM((3, HR, CW), BF), pltpu.VMEM((3, HR, CW), BF), pltpu.VMEM((3, HR, CW), BF),
                pltpu.VMEM((2, 3, HR, CW), BF), pltpu.VMEM((2, 3, HR, CW), BF),
                pltpu.VMEM((3, 3, dr, CW), BF), pltpu.VMEM((3, 3, dr, CW), BF), pltpu.VMEM((3, 3, dr, CW), BF),
                pltpu.VMEM((3, 3, dr, CW), BF), pltpu.VMEM((3, 3, dr, CW), BF), pltpu.VMEM((3, 3, dr, CW), BF),
                pltpu.VMEM((3, dr, CW), BF),
                pltpu.SemaphoreType.DMA((N, 16)), pltpu.SemaphoreType.DMA((N, 16)), pltpu.SemaphoreType.DMA((2,)),
                pltpu.SemaphoreType.DMA((2,)), pltpu.SemaphoreType.DMA((TILES,)), pltpu.SemaphoreType.DMA((3,)),
                pltpu.SemaphoreType.DMA((9,)), pltpu.SemaphoreType.DMA((2, 3)), pltpu.SemaphoreType.DMA((2, 2)),
                pltpu.SemaphoreType.DMA((3, 4)), pltpu.SemaphoreType.DMA((2, 3, 6)), pltpu.SemaphoreType.DMA((4,)),
                pltpu.SemaphoreType.DMA((2,)), pltpu.SemaphoreType.DMA,
            ],
            compiler_params=pltpu.CompilerParams(collective_id=0, has_side_effects=True, vmem_limit_bytes=67043328),
            name="stack",
        )(x, dy, own)
        by_x, og, od = outs[:3]
        back = lambda q: og[:, q].reshape(layers, C, dr, nx, BW).transpose(0, 2, 3, 1, 4).reshape(layers, dr, ff)
        return by_x, back(0), back(1), od

    states, cut = P(("rep", "r", "s"), None, None), P(None, "s", None)
    return jax.shard_map(
        step,
        mesh=mesh,
        in_specs=(states, states) + (cut,) * 3,
        out_specs=(states,) + (P("rep", "s", None),) * 3,
        check_vma=False,
    )
```

```python
import functools

import jax
import jax.numpy as jnp
from jax import lax
from jax.experimental import pallas as pl
from jax.experimental.pallas import tpu as pltpu
from jax.sharding import PartitionSpec as P

BF, F32 = jnp.bfloat16, jnp.float32
MESH = pl.DeviceIdType.MESH
CORES = 2
BW = 128
TILES = 2
SUB = 4
G_, U_, D_ = 0, 1, 2


def dot(a, b, ca=1, cb=0):
    return lax.dot_general(a, b, (((ca,), (cb,)), ((), ())), preferred_element_type=F32)


def when(condition, f):
    if isinstance(condition, bool):
        if condition:
            f()
    else:
        pl.when(condition)(f)


def kernel(dims, x_ref, dy_ref, wg_ref, wu_ref, wd_ref,
           by_x, og, ou, od, G, WDO, ST, PT, A0T, H1,
           a_nat, a_t, dyv, acc, wbuf, dgu, pt, stb, own_v,
           s_send, d_recv, own32, r32, l32, s_u1, s_pr, s_pl, u2r, u2l, ra, rb, rc, rd, v, ya, yb, yc, f_out,
           g_send, g_recv, w_sem, st_sem, pt_sem, ld_sem, rs_send, d_sem, x_sem, rc_sem, y_sem, o_sem, od_send, od_recv,
           own_sem, own_out, ex_send, ex_recv):
    nx, ny, C, T, D = dims
    TM = T // TILES
    N = 2 * C
    DR = D // (CORES * nx)
    HR, QR = DR // 2, DR // 4
    CW = nx * BW
    DH = D // 2

    s, y = lax.axis_index("s"), lax.axis_index("r")
    X, k = lax.div(s, CORES), lax.rem(s, CORES)
    at = lambda xx, kk: CORES * lax.rem(xx, nx) + kk
    right, left = {"s": at(X + 1, k)}, {"s": at(X + nx - 1, k)}
    sib = {"s": at(X, 1 - k)}
    up, down = {"r": lax.rem(y + 1, ny)}, {"r": lax.rem(y + ny - 1, ny)}

    barrier = pltpu.get_barrier_semaphore()
    for who in (right, left, sib, up, down):
        pl.semaphore_signal(barrier, inc=1, device_id=who, device_id_type=MESH)
    pl.semaphore_wait(barrier, 5)

    def remote(src, dst, ss, rs, who):
        return pltpu.make_async_remote_copy(src_ref=src, dst_ref=dst, send_sem=ss, recv_sem=rs, device_id=who, device_id_type=MESH)

    def arrived(dst, rs):
        pltpu.make_async_copy(dst, dst, rs).wait()

    pL, pR, pO = at(X + nx - 1, k), at(X + 1, k), at(X + 2, k)
    par = lax.rem(y, 2)
    mine, other = par * HR, (1 - par) * HR

    def rows(base, q):
        return pl.ds(pl.multiple_of(base + q * QR, QR), QR)

    def out_copy(t, n):
        full = pl.ds(0, DR)
        spec = {
            0: (None, rows(mine, 0), right), 1: (None, rows(mine, 1), right),
            2: (None, rows(mine, 1), left), 3: (None, rows(mine, 0), left),
            4: (pL, rows(mine, 0), right), 5: (pR, rows(mine, 1), left),
            6: (pL, rows(mine, 0), up), 7: (pR, rows(mine, 0), up), 8: (pO, rows(mine, 0), up),
            9: (pL, rows(mine, 1), down), 10: (pR, rows(mine, 1), down), 11: (pO, rows(mine, 1), down),
            12: (None, full, sib), 13: (pL, full, sib), 14: (pR, full, sib), 15: (pO, full, sib),
        }
        j, r, who = spec[t]
        src = own_v.at[lax.rem(n, 4), :, r, :] if j is None else G.at[n, :, j, r, :]
        return remote(src, G.at[n, :, s if j is None else j, r, :], g_send.at[n, t], g_recv.at[n, t], who)

    def in_wait(t, n):
        full = pl.ds(0, DR)
        oL, oR, oO, oS = at(X + nx - 1, 1 - k), at(X + 1, 1 - k), at(X + 2, 1 - k), at(X, 1 - k)
        spec = {
            0: (pL, rows(mine, 0)), 1: (pL, rows(mine, 1)), 2: (pR, rows(mine, 1)), 3: (pR, rows(mine, 0)),
            4: (pO, rows(mine, 0)), 5: (pO, rows(mine, 1)),
            6: (pL, rows(other, 0)), 7: (pR, rows(other, 0)), 8: (pO, rows(other, 0)),
            9: (pL, rows(other, 1)), 10: (pR, rows(other, 1)), 11: (pO, rows(other, 1)),
            12: (oS, full), 13: (oL, full), 14: (oR, full), 15: (oO, full),
        }
        j, r = spec[t]
        arrived(G.at[n, :, j, r, :], g_recv.at[n, t])

    def named(f):
        def run(*args):
            with jax.named_scope(f.__name__):
                return f(*args)
        return run

    def stage(f):
        return lambda n: when((n >= 0) & (n < N) if not isinstance(n, int) else 0 <= n < N, lambda: named(f)(n))

    def starts(n, *ts):
        for t in ts:
            out_copy(t, n).start()

    def layer_of(n):
        if isinstance(n, int):
            return n // C, n % C
        second = n >= C
        return jnp.where(second, 1, 0), jnp.where(second, n - C, n)

    def block_cols(j, c):
        return pl.ds(pl.multiple_of((j * C + c) * BW, BW), BW)

    def half_block(h):
        o = jnp.where(h >= C, 1, 0)
        return o, pl.ds(pl.multiple_of(HR * (h - C * o), HR), HR)

    def core_cols(core):
        return pl.ds(pl.multiple_of(core * DH, DH), DH)

    def exchange(layer):
        mine_ = pl.ds(pl.multiple_of(k * C * HR, HR), C * HR)
        return remote(wd_ref.at[layer, :, core_cols(1 - k)], WDO.at[layer, mine_], ex_send.at[layer], ex_recv.at[layer], sib)

    def exchanged(layer):
        theirs = pl.ds(pl.multiple_of((1 - k) * C * HR, HR), C * HR)
        arrived(WDO.at[layer, theirs], ex_recv.at[layer])

    def free_own(n):
        for t in (0, 1, 2, 3, 12):
            out_copy(t, n).wait_send()

    def own_down(n):
        slot, (layer, c) = lax.rem(n, 4), layer_of(n)
        for e in range(2):
            h = 2 * c + e
            o, r = half_block(h)
            dst, sem = own_v.at[slot, D_, pl.ds(e * HR, HR)], own_sem.at[slot]
            far = pl.ds(pl.multiple_of(HR * h, HR), HR)
            pl.when(o == k)(lambda: pltpu.make_async_copy(wd_ref.at[layer, r, core_cols(k)], dst, sem).start())
            pl.when(o != k)(lambda: pltpu.make_async_copy(WDO.at[layer, far], dst, sem).start())

    def own_cols(n):
        slot, (layer, c) = lax.rem(n, 4), layer_of(n)
        for q, w in ((G_, wg_ref), (U_, wu_ref)):
            for j in range(nx):
                pltpu.make_async_copy(w.at[layer, :, block_cols(j, c)], own_v.at[slot, q, :, pl.ds(j * BW, BW)], own_sem.at[slot]).start()

    @stage
    def gS(n):
        when(n >= 4, lambda: free_own(n - 4))
        own_cols(n)
        own_down(n)

    def own_stored(n):
        return pltpu.make_async_copy(own_v.at[lax.rem(n, 4)], G.at[n, :, s], own_out.at[lax.rem(n, 4)])

    @stage
    def gA(n):
        slot = lax.rem(n, 4)
        pltpu.make_async_copy(own_v.at[slot], own_v.at[slot], own_sem.at[slot]).wait()
        starts(n, 0, 2, 1, 3, 12)
        own_stored(n).start()

    @stage
    def gB(n):
        in_wait(0, n)
        starts(n, 4, 6)
        in_wait(2, n)
        starts(n, 5, 10)

    @stage
    def gC(n):
        in_wait(1, n)
        starts(n, 9)
        in_wait(3, n)
        starts(n, 7)

    @stage
    def gD(n):
        in_wait(4, n)
        starts(n, 8)
        in_wait(5, n)
        starts(n, 11)

    @stage
    def gE(n):
        for a, b, t in ((6, 9, 13), (7, 10, 14), (8, 11, 15)):
            in_wait(a, n)
            in_wait(b, n)
            starts(n, t)
        own_stored(n).wait()

    def load_weights(n, slot):
        for p in range(CORES * nx):
            pltpu.make_async_copy(G.at[n, :, p], wbuf.at[slot, :, p], w_sem.at[slot]).start()

    @named
    def wait_weights(slot):
        pltpu.make_async_copy(wbuf.at[slot], wbuf.at[slot], w_sem.at[slot]).wait()

    @stage
    def gF(n):
        for t in (12, 13, 14, 15):
            in_wait(t, n)
        load_weights(n, lax.rem(n, 2))

    def w_cols(slot, q):
        return wbuf[slot, q].reshape(D, CW)

    def w_half(slot, q, h):
        return wbuf[slot, q, pl.ds(h * nx, nx)].reshape(DH, CW)

    def wd_half(slot, h):
        return jnp.concatenate([wbuf[slot, D_, CORES * j + h] for j in range(nx)], axis=0)

    def tile(i, n=None):
        n = TM if n is None else n
        return pl.ds(pl.multiple_of(i * n, n), n)

    def rel(j):
        return lax.rem(X + j, nx)

    def lane_lhs(lane):
        return jnp.concatenate([a_t[rel(j), lane] for j in range(nx)], axis=0)

    def grad(q, lane):
        if q == D_:
            lhs = jnp.concatenate([pt[rel(j)] for j in range(nx)], axis=0)
            return dot(lhs, dyv[lane])
        return dot(lane_lhs(lane), dgu[q])

    def d_copy(q, m):
        return remote(s_send.at[q], d_recv.at[lax.rem(m, 2), q], rs_send.at[q], d_sem.at[lax.rem(m, 2), q], sib)

    def send_lane(q, m):
        s_send[q] = grad(q, 1 - k).astype(BF).reshape(nx, DR, CW)

    @named
    def send_lanes(m):
        def f():
            for q in (D_, G_, U_):
                d_copy(q, m - 1).wait_send()
        when(m > 0, f)
        when(m >= 3, lambda: y3_wait(m - 3))
        send_lane(D_, m)
        y3_add(m - 3)
        send_lane(G_, m)
        d_copy(D_, m).start()
        d_copy(G_, m).start()
        when(m >= 3, lambda: y3_out(m - 3))
        when(m >= 1, lambda: x2_wait(m - 1))
        send_lane(U_, m)
        x2_add(m - 1)
        d_copy(U_, m).start()
        when(m >= 1, lambda: x2_out(m - 1))

    lo, hi = pl.ds(0, HR), pl.ds(HR, HR)

    def x_copy(t, m):
        two, three = lax.rem(m, 2), lax.rem(m, 3)
        src, dst, sem, who = {
            0: (s_u1.at[:, lo], ra.at[two], x_sem.at[two, 0], right),
            1: (s_u1.at[:, hi], rb.at[two], x_sem.at[two, 1], left),
            2: (s_pr, rc.at[three, :, hi], rc_sem.at[three, 0], right),
            3: (s_pl, rd.at[three, :, lo], rc_sem.at[three, 1], left),
            4: (u2r, rc.at[three, :, lo], rc_sem.at[three, 2], right),
            5: (u2l, rd.at[three, :, hi], rc_sem.at[three, 3], left),
        }[t]
        return remote(src, dst, rs_send.at[3 + t], sem, who)

    def x_wait(t, m):
        two, three = lax.rem(m, 2), lax.rem(m, 3)
        dst, sem = {
            0: (ra.at[two], x_sem.at[two, 0]),
            1: (rb.at[two], x_sem.at[two, 1]),
            2: (rc.at[three, :, hi], rc_sem.at[three, 0]),
            3: (rd.at[three, :, lo], rc_sem.at[three, 1]),
            4: (rc.at[three, :, lo], rc_sem.at[three, 2]),
            5: (rd.at[three, :, hi], rc_sem.at[three, 3]),
        }[t]
        arrived(dst, sem)

    def y_copy(t, m):
        three = lax.rem(m, 3)
        src, dst, who = {
            0: (v.at[three, :, lo], ya.at[three, :, lo], up),
            1: (v.at[three, :, hi], ya.at[three, :, hi], up),
            2: (v.at[three, :, hi], yb.at[three, :, hi], down),
            3: (v.at[three, :, lo], yb.at[three, :, lo], down),
            4: (ya.at[three, :, lo], yc.at[three, :, lo], up),
            5: (yb.at[three, :, hi], yc.at[three, :, hi], down),
        }[t]
        return remote(src, dst, y_sem.at[0, three, t], y_sem.at[1, three, t], who)

    def y_wait(t, m):
        three = lax.rem(m, 3)
        dst = {0: ya.at[three, :, lo], 1: ya.at[three, :, hi], 2: yb.at[three, :, hi], 3: yb.at[three, :, lo],
               4: yc.at[three, :, lo], 5: yc.at[three, :, hi]}[t]
        arrived(dst, y_sem.at[1, three, t])

    @named
    def keep_lanes(m):
        two = lax.rem(m, 2)

        def f():
            for t in range(4):
                x_copy(t, m - 1).wait_send()
        when(m > 0, f)
        for q in (D_, G_, U_):
            arrived(d_recv.at[two, q], d_sem.at[two, q])
        for q in (D_, G_, U_):
            total = (grad(q, k) + d_recv[two, q].reshape(CW, CW).astype(F32)).reshape(nx, DR, CW)
            own32[two, q] = total[0]
            r32[q] = total[1, :HR]
            s_pr[q] = total[1, HR:].astype(BF)
            s_u1[q] = total[2].astype(BF)
            s_pl[q] = total[3, :HR].astype(BF)
            l32[q] = total[3, HR:]

    @named
    def x1(m):
        for t in range(4):
            x_copy(t, m).start()

    def slot_of(m, n):
        return lax.rem(m + n, n)

    @named
    def x2_wait(m):
        x_wait(0, m)
        x_wait(1, m)

        def f():
            x_copy(4, m - 1).wait_send()
            x_copy(5, m - 1).wait_send()
        when(m > 0, f)

    def x2_add(m):
        two = slot_of(m, 2)
        for q in range(3):
            u2r[q] = (r32[q] + ra[two, q].astype(F32)).astype(BF)
            u2l[q] = (l32[q] + rb[two, q].astype(F32)).astype(BF)

    def x2_out(m):
        x_copy(4, m).start()
        x_copy(5, m).start()

    def x2(m):
        x2_wait(m)
        x2_add(m)
        x2_out(m)

    @named
    def x3(m):
        for t in (2, 3, 4, 5):
            x_wait(t, m)
        two, three = lax.rem(m, 2), lax.rem(m, 3)
        for q in range(3):
            v[three, q] = (own32[two, q] + rc[three, q].astype(F32) + rd[three, q].astype(F32)).astype(BF)
        for t in range(4):
            y_copy(t, m).start()

    @named
    def y2(m):
        y_wait(0, m)
        y_copy(4, m).start()
        y_wait(2, m)
        y_copy(5, m).start()

    def where_m(m):
        first = m < C
        return jnp.where(first, 1, 0), jnp.where(first, m, m - C)

    def cols_out(q, m):
        layer, c = where_m(m)
        return [pltpu.make_async_copy(f_out.at[q, :, pl.ds(j * BW, BW)], (og, ou)[q].at[layer, :, block_cols(j, c)], o_sem.at[q])
                for j in range(nx)]

    def od_each(m, local, far):
        layer, c = where_m(m)
        for e in range(2):
            o, r = half_block(2 * c + e)
            src, dst = f_out.at[D_, pl.ds(e * HR, HR)], od.at[layer, r, core_cols(k)]
            pl.when(o == k)(functools.partial(local, pltpu.make_async_copy(src, dst, o_sem.at[2 + e])))
            pl.when(o != k)(functools.partial(far, remote(src, dst, od_send.at[e], od_recv, sib)))

    @named
    def out_done(m):
        for q in (G_, U_):
            pltpu.make_async_copy(f_out.at[q], f_out.at[q], o_sem.at[q]).wait()
        od_each(m, lambda c: c.wait(), lambda c: c.wait_send())

    @named
    def y3_wait(m):
        for t in (1, 3, 4, 5):
            y_wait(t, m)
        when(m > 0, lambda: out_done(m - 1))

    def y3_add(m):
        three = slot_of(m, 3)
        for q in range(3):
            a = v[three, q].astype(F32) + yc[three, q].astype(F32)
            b = ya[three, q].astype(F32) + yb[three, q].astype(F32)
            f_out[q] = (a + b).astype(BF)

    @named
    def y3_out(m):
        for t in range(6):
            y_copy(t, m).wait_send()
        for q in (G_, U_):
            for c_ in cols_out(q, m):
                c_.start()
        od_each(m, lambda c: c.start(), lambda c: c.start())

    def y3(m):
        y3_wait(m)
        y3_add(m)
        y3_out(m)

    def lagged(f, m):
        when(m >= 0, lambda: f(m))

    def halves(src, dst, r, sem):
        return [pltpu.make_async_copy(src.at[r, pl.ds(h * DH, DH)], dst.at[h, r], sem) for h in range(2)]

    every = pl.ds(0, T)
    for layer in range(2):
        exchange(layer).start()
    own_cols(0)
    for c_ in halves(x_ref.at[0], dyv, every, ld_sem.at[0]):
        c_.start()
    exchanged(0)
    own_down(0)
    gA(0)
    gS(1)
    pltpu.make_async_copy(dyv, dyv, ld_sem.at[0]).wait()

    NT = 4 * TILES
    TN = T // NT

    def both(ref, r):
        return jnp.concatenate([ref[0, r, :], ref[1, r, :]], axis=1)

    def put_a(h, i):
        r = tile(i, TN)
        scale = lax.rsqrt(jnp.mean(h * h, -1, keepdims=True) + 1e-6)
        a = (h * scale).astype(BF)
        a_nat[r, :] = a
        a_t[:, :, :, r] = a.T.reshape(nx, CORES, DR, TN)

    def norm0(i, _):
        r = tile(i, TN)
        put_a(both(dyv, r).astype(F32), i)
        acc[r, :] = jnp.zeros((TN, D), F32)
        return _

    lax.fori_loop(0, NT, norm0, 0)
    a0t_out = pltpu.make_async_copy(a_t, A0T, ld_sem.at[1])
    a0t_out.start()
    exchanged(1)
    gB(0)
    gA(1)
    gS(2)
    gC(0)
    gD(0)
    gB(1)
    gA(2)
    gS(3)
    gC(1)
    gE(0)
    gF(0)
    gD(1)
    gB(2)

    def st_out(tau):
        i = lax.rem(tau, TILES)
        return pltpu.make_async_copy(stb.at[i], ST.at[tau], st_sem.at[i])

    def pt_out(c, i):
        cols = tile(i)
        return pltpu.make_async_copy(pt.at[:, :, cols], PT.at[c, :, :, cols], pt_sem.at[i])

    def gate_up(slot, r):
        a = a_nat[r, :]
        g, u = dot(a, w_cols(slot, G_)), dot(a, w_cols(slot, U_))
        sig = jax.nn.sigmoid(g)
        silu = g * sig
        return silu, u * (sig + silu * (1.0 - sig)), (silu * u).astype(BF)

    def put_pt(p, i):
        pt[:, :, tile(i, TM // SUB)] = p.T.reshape(nx, BW, TM // SUB)

    def fwd(c, carry):
        slot = lax.rem(c, 2)
        wait_weights(slot)

        def one(i, _):
            @pl.when(i == 0)
            def _0():
                gA(c + 3)
                gS(c + 4)
                pl.when(c > 0)(lambda: gE(c + 1))

            @pl.when(i == 1)
            def _1():
                gC(c + 2)
                gD(c + 2)
                pl.when(c == 0)(lambda: gE(c + 1))

            tau = TILES * c + i
            @pl.when(c >= 1)
            def _2():
                st_out(tau - TILES).wait()
                pt_out(c - 1, i).wait()

            with jax.named_scope("fwd_up"):
                for j in range(SUB):
                    e = SUB * i + j
                    r = tile(e, TM // SUB)
                    silu, slope, p = gate_up(slot, r)
                    inner = pl.ds(j * (TM // SUB), TM // SUB)
                    stb[i, 0, inner] = silu
                    stb[i, 1, inner] = slope
                    put_pt(p, e)
                    dgu[0, r, :] = p
                st_out(tau).start()
                pt_out(c, i).start()
            return _

        lax.fori_loop(0, TILES, one, carry)
        gB(c + 3)
        gF(c + 1)
        with jax.named_scope("fwd_down"):
            for h in range(2):
                acc[:, h * DH:(h + 1) * DH] += dot(dgu[0], wd_half(slot, h))
        return carry

    lax.fori_loop(0, C, fwd, 0)
    a0t_out.wait()
    for i in range(TILES):
        st_out(TILES * (C - 1) + i).wait()
        pt_out(C - 1, i).wait()

    def h1_out(i, h):
        r = tile(i, TN)
        return pltpu.make_async_copy(dgu.at[h, r], H1.at[h, r], ld_sem.at[2])

    def norm1(i, _):
        r = tile(i, TN)
        h = (both(dyv, r).astype(F32) + acc[r, :].astype(BF).astype(F32)).astype(BF)
        for e in range(2):
            dgu[e, r, :] = h[:, e * DH:(e + 1) * DH]
            h1_out(i, e).start()
        for c_ in halves(dy_ref.at[0], dyv, r, ld_sem.at[0]):
            c_.start()
        put_a(h.astype(F32), i)
        acc[r, :] = jnp.zeros((TN, D), F32)
        return _

    lax.fori_loop(0, NT, norm1, 0)
    pltpu.make_async_copy(dgu, H1, ld_sem.at[2]).wait()
    pltpu.make_async_copy(dyv, dyv, ld_sem.at[0]).wait()

    def d_p(slot, r):
        return dot(dyv[0, r, :], wd_half(slot, 0), 1, 1) + dot(dyv[1, r, :], wd_half(slot, 1), 1, 1)

    def put_d(r, dp, silu, slope):
        dgu[G_, r, :] = (dp * slope).astype(BF)
        dgu[U_, r, :] = (dp * silu).astype(BF)

    h1_in = [pltpu.make_async_copy(H1.at[h], a_nat.at[:, pl.ds(h * DH, DH)], ld_sem.at[0]) for h in range(2)]
    a0t_in = pltpu.make_async_copy(A0T, a_t, ld_sem.at[1])
    x_in = pltpu.make_async_copy(x_ref.at[0], a_nat, ld_sem.at[2])

    def st_load(c):
        for i in range(TILES):
            for e in range(2):
                pltpu.make_async_copy(ST.at[TILES * c + i, e], stb.at[i, e], st_sem.at[i]).start()

    def st_wait(i):
        pltpu.make_async_copy(stb.at[i], stb.at[i], st_sem.at[i]).wait()

    def pt_in(c):
        return pltpu.make_async_copy(PT.at[c], pt, pt_sem.at[0])

    def norm_back(h, d, through):
        scale = lax.rsqrt(jnp.mean(h * h, -1, keepdims=True) + 1e-6)
        along = jnp.sum(d * h, -1, keepdims=True) * (scale * scale * scale) * (1.0 / D)
        return (through + (d * scale - h * along)).astype(BF)

    def middle():
        pltpu.make_async_copy(a_nat, a_nat, ld_sem.at[0]).wait()

        def mid(i, _):
            with jax.named_scope("mid"):
                r = tile(i, TN)
                out = norm_back(a_nat[r, :].astype(F32), acc[r, :], both(dyv, r).astype(F32))
                for e in range(2):
                    dyv[e, r, :] = out[:, e * DH:(e + 1) * DH]
                acc[r, :] = jnp.zeros((TN, D), F32)
            return _

        lax.fori_loop(0, NT, mid, 0)
        x_in.start()
        a0t_in.wait()

    at_hook = {
        0: {0: [(gA, 3), (gE, 1), (gS, 4)], 1: [(gS, 6)]},
        1: {0: [(gC, 2), (gD, 2), (gB, 3), (gA, 4), (gS, 5)], 1: [(gC, 5), (gA, 6)], 2: [(gD, 6), (gE, 5)], 3: [(gE, 6)]},
        2: {},
        3: {0: [(gE, 2), (gC, 3), (gD, 3), (gB, 4), (gA, 5)], 1: [(gB, 6), (gC, 6)]},
        4: {0: [(gC, 4)], 1: [(gD, 5)]},
        5: {0: [(gD, 4), (gE, 3), (gB, 5)], 1: [(gE, 4)]},
    }

    def hook(h, m):
        for step, todo in at_hook[h].items():
            @pl.when(m == step)
            def _(todo=todo):
                for f, n in todo:
                    f(C + n)

    def bwd(m, carry):
        slot = lax.rem(m + 1, 2)
        last = m == C - 1
        first_layer = m >= C
        pl.when(m == C)(middle)
        wait_weights(slot)

        @pl.when(first_layer & (m < 2 * C - 1))
        def _():
            load_weights(m + 1 - C, 1 - slot)

        hook(0, m)

        @pl.when(jnp.logical_not(first_layer))
        def _():
            def one(i, _):
                @pl.when(i == 1)
                def _1():
                    hook(1, m)

                with jax.named_scope("bwd1_tile"):
                    for j in range(SUB):
                        e = SUB * i + j
                        r = tile(e, TM // SUB)
                        silu, slope, p = gate_up(slot, r)
                        put_pt(p, e)
                        put_d(r, d_p(slot, r), silu, slope)
                return _

            lax.fori_loop(0, TILES, one, 0)

        @pl.when(first_layer)
        def _():
            def one(i, _):
                st_wait(i)
                with jax.named_scope("bwd0_tile"):
                    r = tile(i)
                    put_d(r, d_p(slot, r), stb[i, 0], stb[i, 1])
                return _

            lax.fori_loop(0, TILES, one, 0)
            pt_in(m - C).wait()

        hook(2, m)

        @pl.when(last)
        def _():
            for c_ in h1_in:
                c_.start()
            load_weights(0, 1 - slot)

        @pl.when((m >= C - 1) & (m < 2 * C - 1))
        def _():
            st_load(m + 1 - C)

        send_lanes(m)
        lagged(y2, m - 2)
        hook(3, m)
        pl.when(m < C - 1)(lambda: gF(C + 1 + m))

        def d_a(i):
            with jax.named_scope("da_tile"):
                r = tile(i)
                for h in range(2):
                    acc[r, h * DH:(h + 1) * DH] += (
                        dot(dgu[G_, r, :], w_half(slot, G_, h), 1, 1) + dot(dgu[U_, r, :], w_half(slot, U_, h), 1, 1))

        def rest(i, _):
            d_a(i)

            @pl.when(i == 0)
            def _0():
                hook(4, m)
                keep_lanes(m)
                x1(m)
                hook(5, m)
                pl.when((m >= C - 1) & (m < 2 * C - 1))(lambda: pt_in(m + 1 - C).start())
                pl.when(last)(a0t_in.start)
            return _

        lax.fori_loop(0, TILES, rest, 0)
        lagged(x3, m - 1)
        return carry

    lax.fori_loop(0, 2 * C, bwd, 0)

    x_in.wait()
    M = 2 * C
    x2(M - 1)
    y2(M - 2)

    def by_out(i):
        r = tile(i, TN)
        return pltpu.make_async_copy(a_nat.at[r], by_x.at[0, r], ld_sem.at[0])

    def last_norm(i, _):
        r = tile(i, TN)
        a_nat[r, :] = norm_back(a_nat[r, :].astype(F32), acc[r, :], both(dyv, r).astype(F32))
        by_out(i).start()
        return _

    lax.fori_loop(0, NT, last_norm, 0)
    x3(M - 1)
    y3(M - 3)
    y3(M - 2)
    y2(M - 1)
    y3(M - 1)
    pltpu.make_async_copy(a_nat, by_x.at[0], ld_sem.at[0]).wait()
    out_done(M - 1)
    for q in range(3):
        d_copy(q, M - 1).wait_send()
    for t in range(6):
        x_copy(t, M - 1).wait_send()
    arrived(od.at[:, :, pl.ds(0, DH)], od_recv)
    for layer in range(2):
        exchange(layer).wait_send()

    def sent(n, _):
        for t in (4, 5, 6, 7, 8, 9, 10, 11, 13, 14, 15):
            out_copy(t, n).wait_send()
        pl.when(n >= N - 4)(lambda: free_own(n))
        return _

    lax.fori_loop(0, N, sent, 0)


def solution(mesh):
    nx, ny = mesh.shape["s"] // CORES, mesh.shape["r"]

    def step(x, dy, w_gate, w_up, w_down):
        layers, dr, ff = w_gate.shape
        _, T, D = x.shape
        C = ff // (nx * BW)
        N, CW, DH, HR = layers * C, nx * BW, D // 2, dr // 2
        TM = T // TILES

        hbm = pl.BlockSpec(memory_space=pltpu.HBM)
        shape = jax.ShapeDtypeStruct
        outs = pl.pallas_call(
            functools.partial(kernel, (nx, ny, C, T, D)),
            out_shape=[
                shape((1, T, D), BF), shape(w_gate.shape, BF), shape(w_up.shape, BF), shape(w_down.shape, BF),
                shape((N, 3, CORES * nx, dr, CW), BF), shape((layers, C * BW, DH), BF),
                shape((TILES * C, 2, TM, CW), F32), shape((C, nx, BW, T), BF),
                shape((nx, CORES, dr, T), BF), shape((2, T, DH), BF),
            ],
            in_specs=[hbm] * 5,
            out_specs=[hbm] * 10,
            scratch_shapes=[
                pltpu.VMEM((T, D), BF), pltpu.VMEM((nx, CORES, dr, T), BF), pltpu.VMEM((2, T, DH), BF), pltpu.VMEM((T, D), F32),
                pltpu.VMEM((2, 3, CORES * nx, dr, CW), BF), pltpu.VMEM((2, T, CW), BF), pltpu.VMEM((nx, BW, T), BF),
                pltpu.VMEM((TILES, 2, TM, CW), F32), pltpu.VMEM((4, 3, dr, CW), BF),
                pltpu.VMEM((3, nx, dr, CW), BF), pltpu.VMEM((2, 3, nx, dr, CW), BF), pltpu.VMEM((2, 3, dr, CW), F32),
                pltpu.VMEM((3, HR, CW), F32), pltpu.VMEM((3, HR, CW), F32), pltpu.VMEM((3, dr, CW), BF),
                pltpu.VMEM((3, HR, CW), BF), pltpu.VMEM((3, HR, CW), BF), pltpu.VMEM((3, HR, CW), BF), pltpu.VMEM((3, HR, CW), BF),
                pltpu.VMEM((2, 3, HR, CW), BF), pltpu.VMEM((2, 3, HR, CW), BF),
                pltpu.VMEM((3, 3, dr, CW), BF), pltpu.VMEM((3, 3, dr, CW), BF), pltpu.VMEM((3, 3, dr, CW), BF),
                pltpu.VMEM((3, 3, dr, CW), BF), pltpu.VMEM((3, 3, dr, CW), BF), pltpu.VMEM((3, 3, dr, CW), BF),
                pltpu.VMEM((3, dr, CW), BF),
                pltpu.SemaphoreType.DMA((N, 16)), pltpu.SemaphoreType.DMA((N, 16)), pltpu.SemaphoreType.DMA((2,)),
                pltpu.SemaphoreType.DMA((2,)), pltpu.SemaphoreType.DMA((TILES,)), pltpu.SemaphoreType.DMA((3,)),
                pltpu.SemaphoreType.DMA((9,)), pltpu.SemaphoreType.DMA((2, 3)), pltpu.SemaphoreType.DMA((2, 2)),
                pltpu.SemaphoreType.DMA((3, 4)), pltpu.SemaphoreType.DMA((2, 3, 6)), pltpu.SemaphoreType.DMA((4,)),
                pltpu.SemaphoreType.DMA((2,)), pltpu.SemaphoreType.DMA,
                pltpu.SemaphoreType.DMA((4,)), pltpu.SemaphoreType.DMA((4,)), pltpu.SemaphoreType.DMA((2,)), pltpu.SemaphoreType.DMA((2,)),
            ],
            compiler_params=pltpu.CompilerParams(collective_id=0, has_side_effects=True, vmem_limit_bytes=67043328),
            name="stack",
        )(x, dy, w_gate, w_up, w_down)
        return tuple(outs[:4])

    states, cut = P(("rep", "r", "s"), None, None), P(None, "s", None)
    return jax.shard_map(
        step,
        mesh=mesh,
        in_specs=(states, states) + (cut,) * 3,
        out_specs=(states,) + (P("rep", "s", None),) * 3,
        check_vma=False,
    )
```

```python
import functools

import jax
import jax.numpy as jnp
from jax import lax
from jax.experimental import pallas as pl
from jax.experimental.pallas import tpu as pltpu
from jax.sharding import PartitionSpec as P

BF, F32 = jnp.bfloat16, jnp.float32
MESH = pl.DeviceIdType.MESH
CORES = 2
BW = 128
TILES = 2
SUB = 4
G_, U_, D_ = 0, 1, 2


def dot(a, b, ca=1, cb=0):
    return lax.dot_general(a, b, (((ca,), (cb,)), ((), ())), preferred_element_type=F32)


def when(condition, f):
    if isinstance(condition, bool):
        if condition:
            f()
    else:
        pl.when(condition)(f)


def kernel(dims, x_ref, dy_ref, wg_ref, wu_ref, wd_ref,
           by_x, og, ou, od, G, WDO, ST, PT, A0T, H1, DGU,
           a_nat, a_t, dyv, acc, wbuf, dgu, pt, stb, own_v,
           s_send, d_recv, own32, r32, l32, s_u1, s_pr, s_pl, u2r, u2l, ra, rb, rc, rd, v, ya, yb, yc, f_out,
           g_send, g_recv, w_sem, st_sem, pt_sem, ld_sem, rs_send, d_sem, x_sem, rc_sem, ys_sem, yr_sem, o_sem, od_send, od_recv,
           own_sem, own_out, ex_send, ex_recv, dg_sem):
    nx, ny, C, T, D = dims
    TM = T // TILES
    N = 2 * C
    DR = D // (CORES * nx)
    HR, QR = DR // 2, DR // 4
    CW = nx * BW
    DH = D // 2

    s, y = lax.axis_index("s"), lax.axis_index("r")
    X, k = lax.div(s, CORES), lax.rem(s, CORES)
    at = lambda xx, kk: CORES * lax.rem(xx, nx) + kk
    right, left = {"s": at(X + 1, k)}, {"s": at(X + nx - 1, k)}
    sib = {"s": at(X, 1 - k)}
    up, down = {"r": lax.rem(y + 1, ny)}, {"r": lax.rem(y + ny - 1, ny)}

    def remote(src, dst, ss, rs, who):
        return pltpu.make_async_remote_copy(src_ref=src, dst_ref=dst, send_sem=ss, recv_sem=rs, device_id=who, device_id_type=MESH)

    def arrived(dst, rs):
        pltpu.make_async_copy(dst, dst, rs).wait()

    pL, pR, pO = at(X + nx - 1, k), at(X + 1, k), at(X + 2, k)
    others = (at(X + nx - 1, 1 - k), at(X + 1, 1 - k), at(X + 2, 1 - k), at(X, 1 - k))
    par = lax.rem(y, 2)
    mine, other = par * HR, (1 - par) * HR

    def rows(base, q):
        return pl.ds(pl.multiple_of(base + q * QR, QR), QR)

    PARTS = {None: pl.ds(0, 3), 0: pl.ds(0, 2), 1: pl.ds(2, 1)}

    def out_copy(t, n, part=None):
        full = pl.ds(0, DR)
        spec = {
            0: (None, rows(mine, 0), right), 1: (None, rows(mine, 1), right),
            2: (None, rows(mine, 1), left), 3: (None, rows(mine, 0), left),
            4: (pL, rows(mine, 0), right), 5: (pR, rows(mine, 1), left),
            6: (pL, rows(mine, 0), up), 7: (pR, rows(mine, 0), up), 8: (pO, rows(mine, 0), up),
            9: (pL, rows(mine, 1), down), 10: (pR, rows(mine, 1), down), 11: (pO, rows(mine, 1), down),
            12: (None, full, sib), 13: (pL, full, sib), 14: (pR, full, sib), 15: (pO, full, sib),
        }
        j, r, who = spec[t]
        q = PARTS[part]
        src = own_v.at[lax.rem(n, 4), q, r, :] if j is None else G.at[n, q, j, r, :]
        dst = G.at[n, q, s if j is None else j, r, :]
        leaves = g_send.at[lax.rem(n, 4), 0 if j is None else 1]
        return remote(src, dst, leaves, g_recv.at[8 if part == 1 else lax.rem(n, 8), STAGE[t]], who)

    STAGE = (0, 1, 0, 1, 2, 2, 3, 3, 3, 3, 3, 3, 4, 4, 4, 4)

    def in_wait(i, n, part=None):
        q = PARTS[part]
        to = (G.at[n, q, 0, pl.ds(0, HR)],) * 3 + (G.at[n, q, pl.ds(0, 3), pl.ds(0, HR)], G.at[n, q, pl.ds(0, 4)])
        arrived(to[i], g_recv.at[8 if part == 1 else lax.rem(n, 8), i])

    def left_own(n):
        arrived(G.at[n, :, pl.ds(0, 2)], g_send.at[lax.rem(n, 4), 0])

    def left_passed(n):
        arrived(G.at[n, :, pl.ds(0, 5)], g_send.at[lax.rem(n, 4), 1])

    def named(f):
        def run(*args):
            with jax.named_scope(f.__name__):
                return f(*args)
        return run

    def stage(f):
        return lambda n, *part: when((n >= 0) & (n < N) if not isinstance(n, int) else 0 <= n < N, lambda: named(f)(n, *part))

    def starts(n, part, *ts):
        for t in ts:
            out_copy(t, n, part).start()

    def layer_of(n):
        if isinstance(n, int):
            return n // C, n % C
        second = n >= C
        return jnp.where(second, 1, 0), jnp.where(second, n - C, n)

    def block_cols(j, c):
        return pl.ds(pl.multiple_of((j * C + c) * BW, BW), BW)

    def half_block(h):
        o = jnp.where(h >= C, 1, 0)
        return o, pl.ds(pl.multiple_of(HR * (h - C * o), HR), HR)

    def core_cols(core):
        return pl.ds(pl.multiple_of(core * DH, DH), DH)

    def exchange(layer):
        mine_ = pl.ds(pl.multiple_of(k * C * HR, HR), C * HR)
        return remote(wd_ref.at[layer, :, core_cols(1 - k)], WDO.at[layer, mine_], ex_send.at[layer], ex_recv.at[layer], sib)

    def exchanged(layer):
        theirs = pl.ds(pl.multiple_of((1 - k) * C * HR, HR), C * HR)
        arrived(WDO.at[layer, theirs], ex_recv.at[layer])

    def own_down(n, sem):
        slot, (layer, c) = lax.rem(n, 4), layer_of(n)
        for e in range(2):
            h = 2 * c + e
            o, r = half_block(h)
            dst = own_v.at[slot, D_, pl.ds(e * HR, HR)]
            far = pl.ds(pl.multiple_of(HR * h, HR), HR)
            pl.when(o == k)(lambda: pltpu.make_async_copy(wd_ref.at[layer, r, core_cols(k)], dst, sem).start())
            pl.when(o != k)(lambda: pltpu.make_async_copy(WDO.at[layer, far], dst, sem).start())

    def own_cols(n):
        slot, (layer, c) = lax.rem(n, 4), layer_of(n)
        for q, w in ((G_, wg_ref), (U_, wu_ref)):
            for j in range(nx):
                pltpu.make_async_copy(w.at[layer, :, block_cols(j, c)], own_v.at[slot, q, :, pl.ds(j * BW, BW)], own_sem.at[slot]).start()

    @stage
    def gS(n):
        when(n >= 4, lambda: left_own(n - 4))
        own_cols(n)
        own_down(n, own_sem.at[lax.rem(n, 4)])

    def own_stored(n):
        return pltpu.make_async_copy(own_v.at[lax.rem(n, 4)], G.at[n, :, s], own_out.at[lax.rem(n, 4)])

    @stage
    def gA(n):
        slot = lax.rem(n, 4)
        pltpu.make_async_copy(own_v.at[slot], own_v.at[slot], own_sem.at[slot]).wait()
        starts(n, None, 0, 2, 1, 3, 12)
        own_stored(n).start()

    @stage
    def gB(n, part=None):
        when(n >= 4, lambda: left_passed(n - 4))
        in_wait(0, n, part)
        starts(n, part, 4, 5, 6, 10)

    @stage
    def gC(n, part=None):
        in_wait(1, n, part)
        starts(n, part, 9, 7)

    @stage
    def gD(n, part=None):
        in_wait(2, n, part)
        starts(n, part, 8, 11)

    @stage
    def gE(n, part=None):
        in_wait(3, n, part)
        starts(n, part, 13, 14, 15)
        if part != 1:
            own_stored(n).wait()

    def load(n, packets, *parts):
        slot = lax.rem(n, 2)
        for part in parts:
            q = PARTS[part]
            for p in packets:
                pltpu.make_async_copy(G.at[n, q, p], wbuf.at[slot, q, p], w_sem.at[slot, part]).start()

    def wait_weights(slot, part):
        to = wbuf.at[slot, PARTS[part]]
        pltpu.make_async_copy(to, to, w_sem.at[slot, part]).wait()

    @stage
    def gL(n, *parts):
        load(n, (s, pL, pR, pO), *(parts or (0, 1)))

    @stage
    def gF(n, part=None):
        in_wait(4, n, part)
        load(n, others, *((0, 1) if part is None else (part,)))

    def w_cols(slot, q):
        return wbuf[slot, q].reshape(D, CW)

    def w_half(slot, q, h):
        return wbuf[slot, q, pl.ds(h * nx, nx)].reshape(DH, CW)

    def wd_half(slot, h):
        return jnp.concatenate([wbuf[slot, D_, CORES * j + h] for j in range(nx)], axis=0)

    def tile(i, n=None):
        n = TM if n is None else n
        return pl.ds(pl.multiple_of(i * n, n), n)

    def rel(j):
        return lax.rem(X + j, nx)

    def lane_lhs(lane):
        return jnp.concatenate([a_t[rel(j), lane] for j in range(nx)], axis=0)

    def grad(q, lane):
        if q == D_:
            lhs = jnp.concatenate([pt[rel(j)] for j in range(nx)], axis=0)
            return dot(lhs, dyv[lane])
        return dot(lane_lhs(lane), dgu[q])

    def d_copy(q, m):
        return remote(s_send.at[q], d_recv.at[lax.rem(m, 2), q], rs_send.at[0], d_sem.at[lax.rem(m, 2)], sib)

    def send_lane(q, m):
        s_send[q] = grad(q, 1 - k).astype(BF).reshape(nx, DR, CW)

    @named
    def send_lanes(m):
        when(m > 0, lambda: arrived(s_send, rs_send.at[0]))
        send_lane(D_, m)
        send_lane(G_, m)
        d_copy(D_, m).start()
        d_copy(G_, m).start()
        send_lane(U_, m)
        d_copy(U_, m).start()

    lo, hi = pl.ds(0, HR), pl.ds(HR, HR)

    one, two_ = v.at[0], v.at[pl.ds(0, 2)]

    def x_copy(t, m):
        two, three = lax.rem(m, 2), lax.rem(m, 3)
        src, dst, sem, who = {
            0: (s_u1.at[:, lo], ra.at[two], x_sem.at[two], right),
            1: (s_u1.at[:, hi], rb.at[two], x_sem.at[two], left),
            2: (s_pr, rc.at[three, :, hi], rc_sem.at[three], right),
            3: (s_pl, rd.at[three, :, lo], rc_sem.at[three], left),
            4: (u2r, rc.at[three, :, lo], rc_sem.at[three], right),
            5: (u2l, rd.at[three, :, hi], rc_sem.at[three], left),
        }[t]
        return remote(src, dst, rs_send.at[1 if t < 4 else 2], sem, who)

    def y_copy(t, m):
        three = lax.rem(m, 3)
        src, dst, who = {
            0: (v.at[three, :, lo], ya.at[three, :, lo], up),
            1: (v.at[three, :, hi], ya.at[three, :, hi], up),
            2: (v.at[three, :, hi], yb.at[three, :, hi], down),
            3: (v.at[three, :, lo], yb.at[three, :, lo], down),
            4: (ya.at[three, :, lo], yc.at[three, :, lo], up),
            5: (yb.at[three, :, hi], yc.at[three, :, hi], down),
        }[t]
        return remote(src, dst, ys_sem.at[three], yr_sem.at[three, 0 if t in (0, 2) else 1], who)

    @named
    def keep_lanes(m):
        two = lax.rem(m, 2)

        when(m > 0, lambda: arrived(two_, rs_send.at[1]))
        when(m >= 3, lambda: y3_wait(m - 3))
        arrived(d_recv.at[two], d_sem.at[two])
        for q in (D_, G_, U_):
            if q == G_:
                y3_add(m - 3)
            total = (grad(q, k) + d_recv[two, q].reshape(CW, CW).astype(F32)).reshape(nx, DR, CW)
            own32[two, q] = total[0]
            r32[q] = total[1, :HR]
            s_pr[q] = total[1, HR:].astype(BF)
            s_u1[q] = total[2].astype(BF)
            s_pl[q] = total[3, :HR].astype(BF)
            l32[q] = total[3, HR:]

    @named
    def x1(m):
        for t in range(4):
            x_copy(t, m).start()

    def slot_of(m, n):
        return lax.rem(m + n, n)

    @named
    def x2_wait(m):
        arrived(one, x_sem.at[lax.rem(m, 2)])
        when(m > 0, lambda: arrived(one, rs_send.at[2]))

    def x2_add(m):
        two = slot_of(m, 2)
        for q in range(3):
            u2r[q] = (r32[q] + ra[two, q].astype(F32)).astype(BF)
            u2l[q] = (l32[q] + rb[two, q].astype(F32)).astype(BF)

    def x2_out(m):
        x_copy(4, m).start()
        x_copy(5, m).start()

    def x2(m):
        x2_wait(m)
        x2_add(m)
        x2_out(m)

    @named
    def x3(m):
        arrived(two_, rc_sem.at[lax.rem(m, 3)])
        two, three = lax.rem(m, 2), lax.rem(m, 3)
        for q in range(3):
            v[three, q] = (own32[two, q] + rc[three, q].astype(F32) + rd[three, q].astype(F32)).astype(BF)
        for t in (0, 2, 1, 3):
            y_copy(t, m).start()

    @named
    def y2(m):
        arrived(one, yr_sem.at[lax.rem(m, 3), 0])
        y_copy(4, m).start()
        y_copy(5, m).start()

    def where_m(m):
        first = m < C
        return jnp.where(first, 1, 0), jnp.where(first, m, m - C)

    def cols_out(q, m):
        layer, c = where_m(m)
        return [pltpu.make_async_copy(f_out.at[q, :, pl.ds(j * BW, BW)], (og, ou)[q].at[layer, :, block_cols(j, c)], o_sem.at[q])
                for j in range(nx)]

    def od_each(m, local, far):
        layer, c = where_m(m)
        for e in range(2):
            o, r = half_block(2 * c + e)
            src, dst = f_out.at[D_, pl.ds(e * HR, HR)], od.at[layer, r, core_cols(k)]
            pl.when(o == k)(functools.partial(local, pltpu.make_async_copy(src, dst, o_sem.at[2 + e])))
            pl.when(o != k)(functools.partial(far, remote(src, dst, od_send.at[e], od_recv, sib)))

    @named
    def out_done(m):
        for q in (G_, U_):
            pltpu.make_async_copy(f_out.at[q], f_out.at[q], o_sem.at[q]).wait()
        od_each(m, lambda c: c.wait(), lambda c: c.wait_send())

    @named
    def y3_wait(m):
        arrived(two_, yr_sem.at[lax.rem(m, 3), 1])
        when(m > 0, lambda: out_done(m - 1))

    def y3_add(m):
        three = slot_of(m, 3)
        for q in range(3):
            a = v[three, q].astype(F32) + yc[three, q].astype(F32)
            b = ya[three, q].astype(F32) + yb[three, q].astype(F32)
            f_out[q] = (a + b).astype(BF)

    @named
    def y3_out(m):
        arrived(v, ys_sem.at[lax.rem(m, 3)])
        for q in (G_, U_):
            for c_ in cols_out(q, m):
                c_.start()
        od_each(m, lambda c: c.start(), lambda c: c.start())

    def y3(m):
        y3_wait(m)
        y3_add(m)
        y3_out(m)

    def lagged(f, m):
        when(m >= 0, lambda: f(m))

    def halves(src, dst, r, sem):
        return [pltpu.make_async_copy(src.at[r, pl.ds(h * DH, DH)], dst.at[h, r], sem) for h in range(2)]

    every = pl.ds(0, T)
    own_cols(0)
    for c_ in halves(x_ref.at[0], dyv, every, ld_sem.at[0]):
        c_.start()

    barrier = pltpu.get_barrier_semaphore()
    for who in (right, left, sib, up, down):
        pl.semaphore_signal(barrier, inc=1, device_id=who, device_id_type=MESH)
    with jax.named_scope("entry"):
        pl.semaphore_wait(barrier, 5)

    for layer in range(2):
        exchange(layer).start()
    first = own_v.at[0, PARTS[0]]
    with jax.named_scope("own_wait"):
        pltpu.make_async_copy(first, first, own_sem.at[0]).wait()
    starts(0, 0, 0, 2, 1, 3, 12)
    own_cols(1)
    named(exchanged)(0)
    own_down(0, ld_sem.at[2])
    own_down(1, own_sem.at[1])
    pltpu.make_async_copy(dyv, dyv, ld_sem.at[0]).wait()

    NT = 4 * TILES
    TN = T // NT

    def both(ref, r):
        return jnp.concatenate([ref[0, r, :], ref[1, r, :]], axis=1)

    def put_a(h, i):
        r = tile(i, TN)
        scale = lax.rsqrt(jnp.mean(h * h, -1, keepdims=True) + 1e-6)
        a = (h * scale).astype(BF)
        a_nat[r, :] = a
        a_t[:, :, :, r] = a.T.reshape(nx, CORES, DR, TN)

    def norm0(i, _):
        r = tile(i, TN)
        put_a(both(dyv, r).astype(F32), i)
        acc[r, :] = jnp.zeros((TN, D), F32)
        return _

    lax.fori_loop(0, NT // 4, norm0, 0)
    first = own_v.at[0, PARTS[1]]
    pltpu.make_async_copy(first, first, ld_sem.at[2]).wait()
    starts(0, 1, 0, 2, 1, 3, 12)
    own_stored(0).start()
    lax.fori_loop(NT // 4, NT, norm0, 0)
    a0t_out = pltpu.make_async_copy(a_t, A0T, ld_sem.at[1])
    a0t_out.start()
    gB(0, 0)
    gC(0, 0)
    gB(0, 1)
    gC(0, 1)
    gA(1)
    exchanged(1)
    gS(2)
    gD(0, 0)
    gD(0, 1)
    gB(1)
    gA(2)
    gS(3)
    gE(0, 0)
    gL(0, 0)
    gC(1)
    gE(0, 1)
    gL(0, 1)
    gF(0, 0)

    A, B, C_, D__, E, F, L = gA, gB, gC, gD, gE, gF, gL
    fwd_hooks = {
        (0, 0): [(F, 0, 1), (D__, 1), (B, 2)], (0, 1): [(C_, 2), (A, 3)], (0, 2): [(E, 1), (L, 1), (D__, 2)], (0, 3): [(B, 3), (F, 1)],
        (1, 0): [(C_, 3), (E, 2), (L, 2), (A, 4)], (1, 1): [(D__, 3)], (1, 2): [(F, 2), (B, 4)], (1, 3): [(C_, 4), (E, 3), (A, 5)],
        (2, 0): [(L, 3)], (2, 1): [(D__, 4)], (2, 2): [(F, 3), (B, 5)], (2, 3): [(C_, 5), (E, 4), (A, 6)],
        (3, 0): [(L, 4)], (3, 1): [(D__, 5)], (3, 2): [(F, 4), (B, 6)], (3, 3): [(C_, 6), (E, 5), (A, 7)],
        (4, 0): [(L, 5)], (4, 1): [(D__, 6)], (4, 2): [(F, 5), (B, 7)], (4, 3): [(C_, 7), (E, 6), (A, 8)],
        (5, 0): [(L, 6)], (5, 1): [(D__, 7)], (5, 2): [(F, 6), (B, 8)], (5, 3): [(C_, 8), (E, 7), (A, 9)],
        (6, 0): [(L, 7)], (6, 1): [(D__, 8)], (6, 2): [(F, 7), (B, 9)], (6, 3): [(C_, 9), (E, 8), (A, 10)],
    }

    def fwd_hook(h, c):
        for (at_c, at_h), todo in fwd_hooks.items():
            if at_h == h:
                @pl.when(c == at_c)
                def _(todo=todo):
                    for f, *n in todo:
                        f(*n)
                        if f is gA and n[0] + 1 < N:
                            gS(n[0] + 1)

    def st_out(tau):
        i = lax.rem(tau, TILES)
        return pltpu.make_async_copy(stb.at[i], ST.at[tau], st_sem.at[i])

    def pt_out(c, i):
        cols = tile(i)
        return pltpu.make_async_copy(pt.at[:, :, cols], PT.at[c, :, :, cols], pt_sem.at[i])

    def gate_up(slot, r):
        a = a_nat[r, :]
        g, u = dot(a, w_cols(slot, G_)), dot(a, w_cols(slot, U_))
        sig = jax.nn.sigmoid(g)
        silu = g * sig
        return silu, u * (sig + silu * (1.0 - sig)), (silu * u).astype(BF)

    def put_pt(p, i):
        pt[:, :, tile(i, TM // SUB)] = p.T.reshape(nx, BW, TM // SUB)

    def fwd(c, carry):
        slot = lax.rem(c, 2)
        wait_weights(slot, 0)

        fwd_hook(0, c)

        def up_tile(i, _):
            pl.when(i == 1)(lambda: fwd_hook(1, c))

            @pl.when(c >= 1)
            def stored():
                st_out(TILES * (c - 1) + i).wait()
                pt_out(c - 1, i).wait()

            with jax.named_scope("fwd_up"):
                for j in range(SUB):
                    e = SUB * i + j
                    r = tile(e, TM // SUB)
                    silu, slope, p = gate_up(slot, r)
                    inner = pl.ds(j * (TM // SUB), TM // SUB)
                    stb[i, 0, inner] = silu
                    stb[i, 1, inner] = slope
                    put_pt(p, e)
                    dgu[0, r, :] = p
            st_out(TILES * c + i).start()
            pt_out(c, i).start()
            return _

        lax.fori_loop(0, TILES, up_tile, 0)
        fwd_hook(2, c)
        wait_weights(slot, 1)

        @pl.when(c < C - 1)
        def _():
            with jax.named_scope("fwd_down"):
                for h in range(2):
                    acc[:, h * DH:(h + 1) * DH] += dot(dgu[0], wd_half(slot, h))

        @pl.when(c == C - 1)
        def _():
            a0t_out.wait()

            def one(j, _):
                with jax.named_scope("fwd_last"):
                    for e in range(NT // 2):
                        i = NT // 2 * j + e
                        r = tile(i, TN)
                        total = acc[r, :] + jnp.concatenate([dot(dgu[0, r, :], wd_half(slot, h)) for h in range(2)], axis=1)
                        h = (both(dyv, r).astype(F32) + total.astype(BF).astype(F32)).astype(BF)
                        for g in range(2):
                            dgu[g, r, :] = h[:, g * DH:(g + 1) * DH]
                        put_a(h.astype(F32), i)
                        acc[r, :] = jnp.zeros((TN, D), F32)
                r = tile(j, T // 2)
                for g in range(2):
                    pltpu.make_async_copy(dgu.at[g, r], H1.at[g, r], ld_sem.at[2]).start()
                for c_ in halves(dy_ref.at[0], dyv, r, ld_sem.at[0]):
                    c_.start()
                return _

            lax.fori_loop(0, 2, one, 0)

        fwd_hook(3, c)
        return carry

    lax.fori_loop(0, C, fwd, 0)
    for i in range(TILES):
        st_out(TILES * (C - 1) + i).wait()
        pt_out(C - 1, i).wait()
    pltpu.make_async_copy(dgu, H1, ld_sem.at[2]).wait()
    pltpu.make_async_copy(dyv, dyv, ld_sem.at[0]).wait()

    def d_p(slot, r):
        return dot(dyv[0, r, :], wd_half(slot, 0), 1, 1) + dot(dyv[1, r, :], wd_half(slot, 1), 1, 1)

    def put_d(r, dp, silu, slope):
        dgu[G_, r, :] = (dp * slope).astype(BF)
        dgu[U_, r, :] = (dp * silu).astype(BF)

    h1_in = [pltpu.make_async_copy(H1.at[h], a_nat.at[:, pl.ds(h * DH, DH)], ld_sem.at[0]) for h in range(2)]
    a0t_in = pltpu.make_async_copy(A0T, a_t, ld_sem.at[1])
    x_in = pltpu.make_async_copy(x_ref.at[0], a_nat, ld_sem.at[2])

    def st_load(c):
        for i in range(TILES):
            for e in range(2):
                pltpu.make_async_copy(ST.at[TILES * c + i, e], stb.at[i, e], st_sem.at[i]).start()

    def st_wait(i):
        pltpu.make_async_copy(stb.at[i], stb.at[i], st_sem.at[i]).wait()

    def pt_in(c):
        return pltpu.make_async_copy(PT.at[c], pt, pt_sem.at[0])

    def norm_back(h, d, through):
        scale = lax.rsqrt(jnp.mean(h * h, -1, keepdims=True) + 1e-6)
        along = jnp.sum(d * h, -1, keepdims=True) * (scale * scale * scale) * (1.0 / D)
        return (through + (d * scale - h * along)).astype(BF)

    def middle():
        pltpu.make_async_copy(a_nat, a_nat, ld_sem.at[0]).wait()

        def mid(i, _):
            with jax.named_scope("mid"):
                r = tile(i, TN)
                out = norm_back(a_nat[r, :].astype(F32), acc[r, :], both(dyv, r).astype(F32))
                for e in range(2):
                    dyv[e, r, :] = out[:, e * DH:(e + 1) * DH]
                acc[r, :] = jnp.zeros((TN, D), F32)
            return _

        lax.fori_loop(0, NT, mid, 0)
        x_in.start()
        a0t_in.wait()

    at_hook = {
        0: {0: [(gD, 2), (gA, 4), (gS, 5)], 1: [(gD, 4), (gB, 5), (gC, 5), (gE, 3), (gA, 6)], 2: [(gB, 6), (gC, 6)], 3: [(gE, 6)]},
        2: {0: [(gB, 3), (gC, 3), (gE, 2), (gB, 4), (gC, 4), (gA, 5), (gS, 6)], 1: [(gE, 4)], 2: [(gE, 5)]},
        3: {},
        4: {0: [(gD, 3)], 1: [(gD, 5)], 2: [(gD, 6)]},
    }

    def hook(h, m):
        for step, todo in at_hook[h].items():
            @pl.when(m == step)
            def _(todo=todo):
                for f, n in todo:
                    f(C + n)

    def dg_out(c):
        return pltpu.make_async_copy(dgu.at[:, pl.ds(T // 2, T // 2)], DGU.at[c], dg_sem.at[0])

    def d_a(slot, to, base):
        with jax.named_scope("da_tile"):
            r = pl.ds(base, T // 2)
            for h in range(2):
                acc[to:to + T // 2, h * DH:(h + 1) * DH] += (
                    dot(dgu[G_, r, :], w_half(slot, G_, h), 1, 1) + dot(dgu[U_, r, :], w_half(slot, U_, h), 1, 1))

    def bwd(m, carry):
        slot = lax.rem(m + 1, 2)
        last = m == C - 1
        first_layer = m >= C
        pl.when(m == C)(middle)
        wait_weights(slot, 1)

        @pl.when(first_layer & (m < 2 * C - 1))
        def _():
            load(m + 1 - C, range(CORES * nx), 0, 1)

        hook(0, m)

        @pl.when(jnp.logical_not(first_layer))
        def _():
            wait_weights(slot, 0)

            with jax.named_scope("bwd1_tile"):
                for e in range(TILES * SUB):
                    r = tile(e, TM // SUB)
                    silu, slope, p = gate_up(slot, r)
                    put_pt(p, e)
                    put_d(r, d_p(slot, r), silu, slope)

        @pl.when(first_layer)
        def _():
            pl.when(m > C)(lambda: dg_out(m - 1 - C).wait())
            for i in range(TILES):
                st_wait(i)
            with jax.named_scope("bwd0_tile"):
                for e in range(TILES * SUB):
                    r = pl.ds(e * (TM // SUB), TM // SUB)
                    inner = pl.ds((e % SUB) * (TM // SUB), TM // SUB)
                    put_d(r, d_p(slot, r), stb[e // SUB, 0, inner], stb[e // SUB, 1, inner])
            pl.when(m < 2 * C - 1)(lambda: dg_out(m - C).start())
            pt_in(m - C).wait()

        hook(2, m)
        lagged(x3, m - 2)

        @pl.when(last)
        def _():
            for c_ in h1_in:
                c_.start()
            load(0, range(CORES * nx), 0, 1)

        @pl.when((m >= C - 1) & (m < 2 * C - 1))
        def _():
            st_load(m + 1 - C)

        send_lanes(m)
        hook(3, m)

        @pl.when(m < C - 1)
        def _():
            gL(C + 1 + m)
            gF(C + 1 + m)

        pl.when(first_layer)(lambda: wait_weights(slot, 0))
        d_a(slot, 0, 0)
        lagged(x2, m - 1)
        hook(4, m)
        keep_lanes(m)
        x1(m)
        lagged(y2, m - 2)
        when(m >= 3, lambda: y3_out(m - 3))
        pl.when((m >= C - 1) & (m < 2 * C - 1))(lambda: pt_in(m + 1 - C).start())
        pl.when(last)(a0t_in.start)
        pl.when(m < C)(lambda: d_a(slot, T // 2, T // 2))
        return carry

    lax.fori_loop(0, 2 * C, bwd, 0)

    M = 2 * C

    def dg_in(c, half):
        return pltpu.make_async_copy(DGU.at[c], dgu.at[:, pl.ds(half * (T // 2), T // 2)], dg_sem.at[half])

    def late(j, carry):
        slot, half = lax.rem(j, 2), 1 - lax.rem(j, 2)

        @pl.when(j >= 1)
        def _():
            wait_weights(slot, 0)
            dg_in(j - 1, half).wait()

        @pl.when(j < C - 1)
        def _():
            for p in range(CORES * nx):
                pltpu.make_async_copy(G.at[j, PARTS[0], p], wbuf.at[1 - slot, PARTS[0], p], w_sem.at[1 - slot, 0]).start()
            dg_in(j, 1 - half).start()

        d_a(slot, T // 2, pl.multiple_of(half * (T // 2), T // 2))
        pl.when(j == 0)(lambda: x3(M - 2))
        pl.when(j == C - 6)(lambda: x2(M - 1))
        pl.when(j == C - 4)(lambda: y2(M - 2))
        pl.when(j == C - 3)(lambda: x3(M - 1))
        pl.when(j == C - 2)(lambda: y3(M - 3))
        return carry

    lax.fori_loop(0, C, late, 0)

    x_in.wait()

    def by_out(i):
        r = tile(i, TN)
        return pltpu.make_async_copy(a_nat.at[r], by_x.at[0, r], ld_sem.at[0])

    def last_norm(i, _):
        r = tile(i, TN)
        a_nat[r, :] = norm_back(a_nat[r, :].astype(F32), acc[r, :], both(dyv, r).astype(F32))
        by_out(i).start()
        return _

    lax.fori_loop(0, NT // 2, last_norm, 0)
    y2(M - 1)
    lax.fori_loop(NT // 2, NT, last_norm, 0)
    y3(M - 2)

    arrived(s_send, rs_send.at[0])
    arrived(two_, rs_send.at[1])
    arrived(one, rs_send.at[2])
    for layer in range(2):
        exchange(layer).wait_send()
    for n in range(N - 4, N):
        left_own(n)
        left_passed(n)
    pltpu.make_async_copy(a_nat, by_x.at[0], ld_sem.at[0]).wait()
    y3(M - 1)
    out_done(M - 1)
    arrived(od.at[:, :, pl.ds(0, DH)], od_recv)


def solution(mesh):
    nx, ny = mesh.shape["s"] // CORES, mesh.shape["r"]

    def step(x, dy, w_gate, w_up, w_down):
        layers, dr, ff = w_gate.shape
        _, T, D = x.shape
        C = ff // (nx * BW)
        N, CW, DH, HR = layers * C, nx * BW, D // 2, dr // 2
        TM = T // TILES

        hbm = pl.BlockSpec(memory_space=pltpu.HBM)
        shape = jax.ShapeDtypeStruct
        outs = pl.pallas_call(
            functools.partial(kernel, (nx, ny, C, T, D)),
            out_shape=[
                shape((1, T, D), BF), shape(w_gate.shape, BF), shape(w_up.shape, BF), shape(w_down.shape, BF),
                shape((N, 3, CORES * nx, dr, CW), BF), shape((layers, C * BW, DH), BF),
                shape((TILES * C, 2, TM, CW), F32), shape((C, nx, BW, T), BF),
                shape((nx, CORES, dr, T), BF), shape((2, T, DH), BF), shape((C, 2, T // 2, CW), BF),
            ],
            in_specs=[hbm] * 5,
            out_specs=[hbm] * 11,
            scratch_shapes=[
                pltpu.VMEM((T, D), BF), pltpu.VMEM((nx, CORES, dr, T), BF), pltpu.VMEM((2, T, DH), BF), pltpu.VMEM((T, D), F32),
                pltpu.VMEM((2, 3, CORES * nx, dr, CW), BF), pltpu.VMEM((2, T, CW), BF), pltpu.VMEM((nx, BW, T), BF),
                pltpu.VMEM((TILES, 2, TM, CW), F32), pltpu.VMEM((4, 3, dr, CW), BF),
                pltpu.VMEM((3, nx, dr, CW), BF), pltpu.VMEM((2, 3, nx, dr, CW), BF), pltpu.VMEM((2, 3, dr, CW), F32),
                pltpu.VMEM((3, HR, CW), F32), pltpu.VMEM((3, HR, CW), F32), pltpu.VMEM((3, dr, CW), BF),
                pltpu.VMEM((3, HR, CW), BF), pltpu.VMEM((3, HR, CW), BF), pltpu.VMEM((3, HR, CW), BF), pltpu.VMEM((3, HR, CW), BF),
                pltpu.VMEM((2, 3, HR, CW), BF), pltpu.VMEM((2, 3, HR, CW), BF),
                pltpu.VMEM((3, 3, dr, CW), BF), pltpu.VMEM((3, 3, dr, CW), BF), pltpu.VMEM((3, 3, dr, CW), BF),
                pltpu.VMEM((3, 3, dr, CW), BF), pltpu.VMEM((3, 3, dr, CW), BF), pltpu.VMEM((3, 3, dr, CW), BF),
                pltpu.VMEM((3, dr, CW), BF),
                *(pltpu.SemaphoreType.DMA(n) for n in (
                    (4, 2), (9, 5), (2, 2), (2,), (TILES,), (3,), (3,), (2,), (2,), (3,), (3,), (3, 2), (4,), (2,), (), (4,), (4,), (2,), (2,), (2,))),
            ],
            compiler_params=pltpu.CompilerParams(collective_id=0, has_side_effects=True, vmem_limit_bytes=67043328),
            name="stack",
        )(x, dy, w_gate, w_up, w_down)
        return tuple(outs[:4])

    states, cut = P(("rep", "r", "s"), None, None), P(None, "s", None)
    return jax.shard_map(
        step,
        mesh=mesh,
        in_specs=(states, states) + (cut,) * 3,
        out_specs=(states,) + (P("rep", "s", None),) * 3,
        check_vma=False,
    )
```

```python
import functools

import jax
import jax.numpy as jnp
from jax import lax
from jax.experimental import pallas as pl
from jax.experimental.pallas import tpu as pltpu
from jax.sharding import PartitionSpec as P

BF, F32 = jnp.bfloat16, jnp.float32
MESH = pl.DeviceIdType.MESH
CORES = 2
BW = 128
TILES = 2
NH = 256
SUB = 4
G_, U_, D_ = 0, 1, 2


def dot(a, b, ca=1, cb=0):
    return lax.dot_general(a, b, (((ca,), (cb,)), ((), ())), preferred_element_type=F32)


def when(condition, f):
    if isinstance(condition, bool):
        if condition:
            f()
    else:
        pl.when(condition)(f)


def kernel(dims, x_ref, dy_ref, wg_ref, wu_ref, wd_ref,
           by_x, og, ou, od, G, WDO, ST, PT, A0T, H1, DGU,
           a_nat, a_t, dyv, acc, wbuf, dgu, pt, stb, own_v,
           s_send, d_recv, own32, r32, l32, s_u1, s_pr, s_pl, u2r, u2l, ra, rb, rc, rd, v, ya, yb, yc, f_out,
           g_send, g_recv, w_sem, st_sem, pt_sem, ld_sem, rs_send, d_sem, x_sem, rc_sem, ys_sem, yr_sem, o_sem, od_send, od_recv,
           own_sem, own_out, ex_send, ex_recv, dg_sem):
    nx, ny, C, T, D = dims
    TM = T // TILES
    N = 2 * C
    DR = D // (CORES * nx)
    HR, QR = DR // 2, DR // 4
    CW = nx * BW
    DH = D // 2

    s, y = lax.axis_index("s"), lax.axis_index("r")
    X, k = lax.div(s, CORES), lax.rem(s, CORES)
    at = lambda xx, kk: CORES * lax.rem(xx, nx) + kk
    right, left = {"s": at(X + 1, k)}, {"s": at(X + nx - 1, k)}
    sib = {"s": at(X, 1 - k)}
    up, down = {"r": lax.rem(y + 1, ny)}, {"r": lax.rem(y + ny - 1, ny)}

    def remote(src, dst, ss, rs, who):
        return pltpu.make_async_remote_copy(src_ref=src, dst_ref=dst, send_sem=ss, recv_sem=rs, device_id=who, device_id_type=MESH)

    def arrived(dst, rs):
        pltpu.make_async_copy(dst, dst, rs).wait()

    packet = lambda xx: k * nx + lax.rem(xx, nx)
    own, pL, pR, pO = packet(X), packet(X + nx - 1), packet(X + 1), packet(X + 2)
    par = lax.rem(y, 2)
    mine, other = par * HR, (1 - par) * HR

    def rows(base, q):
        return pl.ds(pl.multiple_of(base + q * QR, QR), QR)

    PARTS = {None: pl.ds(0, 3), 0: pl.ds(0, 2), 1: pl.ds(2, 1)}

    def home(n):
        return wbuf.at[n] if n < 2 else G.at[n]

    def kept(n):
        return pltpu.make_async_copy(wbuf.at[n], G.at[n], w_sem.at[n, 0])

    def out_copy(t, n, part=None):
        full = pl.ds(0, DR)
        spec = {
            0: (None, rows(mine, 0), right), 1: (None, rows(mine, 1), right),
            2: (None, rows(mine, 1), left), 3: (None, rows(mine, 0), left),
            4: (pL, rows(mine, 0), right), 5: (pR, rows(mine, 1), left),
            6: (pL, rows(mine, 0), up), 7: (pR, rows(mine, 0), up), 8: (pO, rows(mine, 0), up),
            9: (pL, rows(mine, 1), down), 10: (pR, rows(mine, 1), down), 11: (pO, rows(mine, 1), down),
            12: (None, full, sib), 13: (pL, full, sib), 14: (pR, full, sib), 15: (pO, full, sib),
        }
        j, r, who = spec[t]
        q = PARTS[part]
        src = own_v.at[lax.rem(n, 4), q, r, :] if j is None else home(n).at[q, j, r, :]
        dst = home(n).at[q, own if j is None else j, r, :]
        leaves = g_send.at[lax.rem(n, 4), 0 if j is None else 1]
        return remote(src, dst, leaves, g_recv.at[8 if part == 1 else lax.rem(n, 8), STAGE[t]], who)

    STAGE = (0, 1, 0, 1, 2, 2, 3, 3, 3, 3, 3, 3, 4, 4, 4, 4)

    def in_wait(i, n, part=None):
        q = PARTS[part]
        to = (G.at[n, q, 0, pl.ds(0, HR)],) * 3 + (G.at[n, q, pl.ds(0, 3), pl.ds(0, HR)], G.at[n, q, pl.ds(0, 4)])
        arrived(to[i], g_recv.at[8 if part == 1 else lax.rem(n, 8), i])

    def left_own(n):
        arrived(G.at[n, :, pl.ds(0, 2)], g_send.at[lax.rem(n, 4), 0])

    def left_passed(n):
        arrived(G.at[n, :, pl.ds(0, 5)], g_send.at[lax.rem(n, 4), 1])

    def named(f):
        def run(*args):
            with jax.named_scope(f.__name__):
                return f(*args)
        return run

    def stage(f):
        return lambda n, *part: when((n >= 0) & (n < N) if not isinstance(n, int) else 0 <= n < N, lambda: named(f)(n, *part))

    def starts(n, part, *ts):
        for t in ts:
            out_copy(t, n, part).start()

    def layer_of(n):
        if isinstance(n, int):
            return n // C, n % C
        second = n >= C
        return jnp.where(second, 1, 0), jnp.where(second, n - C, n)

    def block_cols(j, c):
        return pl.ds(pl.multiple_of((j * C + c) * BW, BW), BW)

    def half_block(h):
        o = jnp.where(h >= C, 1, 0)
        return o, pl.ds(pl.multiple_of(HR * (h - C * o), HR), HR)

    def core_cols(core):
        return pl.ds(pl.multiple_of(core * DH, DH), DH)

    def exchange(layer):
        mine_ = pl.ds(pl.multiple_of(k * C * HR, HR), C * HR)
        return remote(wd_ref.at[layer, :, core_cols(1 - k)], WDO.at[layer, mine_], ex_send.at[layer], ex_recv.at[layer], sib)

    def exchanged(layer):
        theirs = pl.ds(pl.multiple_of((1 - k) * C * HR, HR), C * HR)
        arrived(WDO.at[layer, theirs], ex_recv.at[layer])

    def own_down(n, sem):
        slot, (layer, c) = lax.rem(n, 4), layer_of(n)
        for e in range(2):
            h = 2 * c + e
            o, r = half_block(h)
            dst = own_v.at[slot, D_, pl.ds(e * HR, HR)]
            far = pl.ds(pl.multiple_of(HR * h, HR), HR)
            pl.when(o == k)(lambda: pltpu.make_async_copy(wd_ref.at[layer, r, core_cols(k)], dst, sem).start())
            pl.when(o != k)(lambda: pltpu.make_async_copy(WDO.at[layer, far], dst, sem).start())

    def own_cols(n):
        slot, (layer, c) = lax.rem(n, 4), layer_of(n)
        for q, w in ((G_, wg_ref), (U_, wu_ref)):
            for j in range(nx):
                pltpu.make_async_copy(w.at[layer, :, block_cols(j, c)], own_v.at[slot, q, :, pl.ds(j * BW, BW)], own_sem.at[slot]).start()

    @stage
    def gS(n):
        when(n >= 4, lambda: left_own(n - 4))
        own_cols(n)
        own_down(n, own_sem.at[lax.rem(n, 4)])

    def own_stored(n):
        return pltpu.make_async_copy(own_v.at[lax.rem(n, 4)], home(n).at[:, own], own_out.at[lax.rem(n, 4)])

    @stage
    def gA(n):
        slot = lax.rem(n, 4)
        pltpu.make_async_copy(own_v.at[slot], own_v.at[slot], own_sem.at[slot]).wait()
        starts(n, None, 0, 2, 1, 3, 12)
        own_stored(n).start()

    @stage
    def gB(n, part=None):
        when(n >= 6, lambda: left_passed(n - 4))
        in_wait(0, n, part)
        starts(n, part, 4, 5, 6, 10)

    @stage
    def gC(n, part=None):
        in_wait(1, n, part)
        starts(n, part, 9, 7)

    @stage
    def gD(n, part=None):
        in_wait(2, n, part)
        starts(n, part, 8, 11)

    @stage
    def gE(n, part=None):
        in_wait(3, n, part)
        starts(n, part, 13, 14, 15)
        if part != 1:
            own_stored(n).wait()

    def lane(core):
        return pl.ds(pl.multiple_of(core * nx, nx), nx)

    def load(n, slot, lanes, *parts):
        for part in parts:
            for core in lanes:
                at_ = (PARTS[part], lane(core))
                pltpu.make_async_copy(G.at[n, *at_], wbuf.at[slot, *at_], w_sem.at[slot, part]).start()

    def wait_weights(slot, part):
        to = wbuf.at[slot, PARTS[part]]
        pltpu.make_async_copy(to, to, w_sem.at[slot, part]).wait()

    @stage
    def gL(n):
        if isinstance(n, int) and n in (2, 3):
            left_passed(n - 2)
            kept(n - 2).wait()
        load(n, lax.rem(n, 2), (k,), 0, 1)

    @stage
    def gF(n, part=None):
        in_wait(4, n, part)
        if isinstance(n, int) and n < 2:
            if part != 0:
                kept(n).start()
        else:
            load(n, lax.rem(n, 2), (1 - k,), 0, 1)

    def w_cols(slot, q, n):
        cols = pl.ds(n * NH, NH)
        return jnp.concatenate([wbuf[slot, q, c * nx + x, :, cols] for x in range(nx) for c in range(CORES)], axis=0)

    def w_half(slot, q, h):
        return jnp.concatenate([wbuf[slot, q, c * nx + h * (nx // 2) + x] for x in range(nx // 2) for c in range(CORES)], axis=0)

    def wd_half(slot, h):
        return wbuf[slot, D_, pl.ds(h * nx, nx)].reshape(CW, DH)

    def tile(i, n=None):
        n = TM if n is None else n
        return pl.ds(pl.multiple_of(i * n, n), n)

    def rel(j):
        return lax.rem(X + j, nx)

    def lane_lhs(lane):
        return jnp.concatenate([a_t[rel(j), lane] for j in range(nx)], axis=0)

    def grad(q, lane):
        if q == D_:
            lhs = jnp.concatenate([pt[rel(j)] for j in range(nx)], axis=0)
            return dot(lhs, dyv[lane])
        return dot(lane_lhs(lane), dgu[q])

    def d_copy(q, m):
        return remote(s_send.at[q], d_recv.at[lax.rem(m, 2), q], rs_send.at[0], d_sem.at[lax.rem(m, 2)], sib)

    def send_lane(q, m):
        s_send[q] = grad(q, 1 - k).astype(BF).reshape(nx, DR, CW)

    @named
    def send_lanes(m):
        when(m > 0, lambda: arrived(s_send, rs_send.at[0]))
        send_lane(D_, m)
        send_lane(G_, m)
        d_copy(D_, m).start()
        d_copy(G_, m).start()
        send_lane(U_, m)
        d_copy(U_, m).start()

    lo, hi = pl.ds(0, HR), pl.ds(HR, HR)

    one, two_ = v.at[0], v.at[pl.ds(0, 2)]

    def x_copy(t, m):
        two, three = lax.rem(m, 2), lax.rem(m, 3)
        src, dst, sem, who = {
            0: (s_u1.at[:, lo], ra.at[two], x_sem.at[two], right),
            1: (s_u1.at[:, hi], rb.at[two], x_sem.at[two], left),
            2: (s_pr, rc.at[three, :, hi], rc_sem.at[three], right),
            3: (s_pl, rd.at[three, :, lo], rc_sem.at[three], left),
            4: (u2r, rc.at[three, :, lo], rc_sem.at[three], right),
            5: (u2l, rd.at[three, :, hi], rc_sem.at[three], left),
        }[t]
        return remote(src, dst, rs_send.at[1 if t < 4 else 2], sem, who)

    def y_copy(t, m):
        three = lax.rem(m, 3)
        src, dst, who = {
            0: (v.at[three, :, lo], ya.at[three, :, lo], up),
            1: (v.at[three, :, hi], ya.at[three, :, hi], up),
            2: (v.at[three, :, hi], yb.at[three, :, hi], down),
            3: (v.at[three, :, lo], yb.at[three, :, lo], down),
            4: (ya.at[three, :, lo], yc.at[three, :, lo], up),
            5: (yb.at[three, :, hi], yc.at[three, :, hi], down),
        }[t]
        return remote(src, dst, ys_sem.at[three], yr_sem.at[three, 0 if t in (0, 2) else 1], who)

    @named
    def keep_lanes(m):
        two = lax.rem(m, 2)

        when(m > 0, lambda: arrived(two_, rs_send.at[1]))
        when(m >= 3, lambda: y3_wait(m - 3))
        arrived(d_recv.at[two], d_sem.at[two])
        for q in (D_, G_, U_):
            if q == G_:
                y3_add(m - 3)
            total = (grad(q, k) + d_recv[two, q].reshape(CW, CW).astype(F32)).reshape(nx, DR, CW)
            own32[two, q] = total[0]
            r32[q] = total[1, :HR]
            s_pr[q] = total[1, HR:].astype(BF)
            s_u1[q] = total[2].astype(BF)
            s_pl[q] = total[3, :HR].astype(BF)
            l32[q] = total[3, HR:]

    @named
    def x1(m):
        for t in range(4):
            x_copy(t, m).start()

    def slot_of(m, n):
        return lax.rem(m + n, n)

    @named
    def x2_wait(m):
        arrived(one, x_sem.at[lax.rem(m, 2)])
        when(m > 0, lambda: arrived(one, rs_send.at[2]))

    def x2_add(m):
        two = slot_of(m, 2)
        for q in range(3):
            u2r[q] = (r32[q] + ra[two, q].astype(F32)).astype(BF)
            u2l[q] = (l32[q] + rb[two, q].astype(F32)).astype(BF)

    def x2_out(m):
        x_copy(4, m).start()
        x_copy(5, m).start()

    def x2(m):
        x2_wait(m)
        x2_add(m)
        x2_out(m)

    @named
    def x3(m):
        arrived(two_, rc_sem.at[lax.rem(m, 3)])
        two, three = lax.rem(m, 2), lax.rem(m, 3)
        for q in range(3):
            v[three, q] = (own32[two, q] + rc[three, q].astype(F32) + rd[three, q].astype(F32)).astype(BF)
        for t in (0, 2, 1, 3):
            y_copy(t, m).start()

    @named
    def y2(m):
        arrived(one, yr_sem.at[lax.rem(m, 3), 0])
        y_copy(4, m).start()
        y_copy(5, m).start()

    def where_m(m):
        first = m < C
        return jnp.where(first, 1, 0), jnp.where(first, m, m - C)

    def cols_out(q, m):
        layer, c = where_m(m)
        return [pltpu.make_async_copy(f_out.at[q, :, pl.ds(j * BW, BW)], (og, ou)[q].at[layer, :, block_cols(j, c)], o_sem.at[q])
                for j in range(nx)]

    def od_each(m, local, far):
        layer, c = where_m(m)
        for e in range(2):
            o, r = half_block(2 * c + e)
            src, dst = f_out.at[D_, pl.ds(e * HR, HR)], od.at[layer, r, core_cols(k)]
            pl.when(o == k)(functools.partial(local, pltpu.make_async_copy(src, dst, o_sem.at[2 + e])))
            pl.when(o != k)(functools.partial(far, remote(src, dst, od_send.at[e], od_recv, sib)))

    @named
    def out_done(m):
        for q in (G_, U_):
            pltpu.make_async_copy(f_out.at[q], f_out.at[q], o_sem.at[q]).wait()
        od_each(m, lambda c: c.wait(), lambda c: c.wait_send())

    @named
    def y3_wait(m):
        arrived(two_, yr_sem.at[lax.rem(m, 3), 1])
        when(m > 0, lambda: out_done(m - 1))

    def y3_add(m):
        three = slot_of(m, 3)
        for q in range(3):
            a = v[three, q].astype(F32) + yc[three, q].astype(F32)
            b = ya[three, q].astype(F32) + yb[three, q].astype(F32)
            f_out[q] = (a + b).astype(BF)

    @named
    def y3_out(m):
        arrived(v, ys_sem.at[lax.rem(m, 3)])
        for q in (G_, U_):
            for c_ in cols_out(q, m):
                c_.start()
        od_each(m, lambda c: c.start(), lambda c: c.start())

    def y3(m):
        y3_wait(m)
        y3_add(m)
        y3_out(m)

    def lagged(f, m):
        when(m >= 0, lambda: f(m))

    def halves(src, dst, r, sem):
        return [pltpu.make_async_copy(src.at[r, pl.ds(h * DH, DH)], dst.at[h, r], sem) for h in range(2)]

    every = pl.ds(0, T)
    own_cols(0)
    for c_ in halves(x_ref.at[0], dyv, every, ld_sem.at[0]):
        c_.start()

    barrier = pltpu.get_barrier_semaphore()
    for who in (right, left, sib, up, down):
        pl.semaphore_signal(barrier, inc=1, device_id=who, device_id_type=MESH)
    with jax.named_scope("entry"):
        pl.semaphore_wait(barrier, 5)

    for layer in range(2):
        exchange(layer).start()
    first = own_v.at[0, PARTS[0]]
    with jax.named_scope("own_wait"):
        pltpu.make_async_copy(first, first, own_sem.at[0]).wait()
    starts(0, 0, 0, 2, 1, 3, 12)
    own_cols(1)
    named(exchanged)(0)
    own_down(0, ld_sem.at[2])
    own_down(1, own_sem.at[1])
    pltpu.make_async_copy(dyv, dyv, ld_sem.at[0]).wait()

    NT = 4 * TILES
    TN = T // NT

    def both(ref, r):
        return jnp.concatenate([ref[0, r, :], ref[1, r, :]], axis=1)

    def put_a(h, r):
        scale = lax.rsqrt(jnp.mean(h * h, -1, keepdims=True) + 1e-6)
        a = (h * scale).astype(BF)
        a_nat[r, :] = a
        a_t[:, :, :, r] = a.T.reshape(nx, CORES, DR, TN)

    def norm0(i, _):
        r = tile(i, TN)
        put_a(both(dyv, r).astype(F32), r)
        acc[r, :] = jnp.zeros((TN, D), F32)
        return _

    lax.fori_loop(0, NT // 4, norm0, 0)
    first = own_v.at[0, PARTS[1]]
    pltpu.make_async_copy(first, first, ld_sem.at[2]).wait()
    starts(0, 1, 0, 2, 1, 3, 12)
    own_stored(0).start()
    lax.fori_loop(NT // 4, NT, norm0, 0)
    a0t_out = pltpu.make_async_copy(a_t, A0T, ld_sem.at[1])
    a0t_out.start()
    gB(0, 0)
    gC(0, 0)
    gB(0, 1)
    gA(1)
    gC(0, 1)
    exchanged(1)
    gS(2)
    gD(0, 0)
    gD(0, 1)
    gE(0, 0)
    gB(1)
    gA(2)
    gS(3)
    gE(0, 1)
    gF(0, 0)

    A, B, C_, D__, E, F, L = gA, gB, gC, gD, gE, gF, gL
    fwd_hooks = {
        (0, 0): [(C_, 1), (F, 0, 1)], (0, 1): [(D__, 1), (B, 2), (A, 3)], (0, 2): [(C_, 2), (E, 1)], (0, 3): [(D__, 2), (F, 1)],
        (1, 0): [(B, 3), (A, 4)], (1, 1): [(C_, 3), (E, 2), (L, 2)], (1, 2): [(D__, 3), (B, 4), (F, 2), (A, 5)], (1, 3): [(C_, 4)],
        (2, 1): [(E, 3), (L, 3), (D__, 4)], (2, 2): [(B, 5), (C_, 5), (F, 3), (A, 6)], (2, 3): [(E, 4)],
        (3, 0): [(L, 4)], (3, 1): [(D__, 5)], (3, 2): [(F, 4), (B, 6), (C_, 6), (A, 7)], (3, 3): [(E, 5)],
        (4, 0): [(L, 5)], (4, 1): [(D__, 6)], (4, 2): [(F, 5), (B, 7), (A, 8)], (4, 3): [(C_, 7), (E, 6)],
        (5, 0): [(L, 6)], (5, 1): [(D__, 7)], (5, 2): [(F, 6), (B, 8), (A, 9)], (5, 3): [(C_, 8), (E, 7)],
        (6, 0): [(L, 7)], (6, 1): [(D__, 8)], (6, 2): [(F, 7), (B, 9), (A, 10)], (6, 3): [(C_, 9), (E, 8)],
    }

    def fwd_hook(h, c):
        for (at_c, at_h), todo in fwd_hooks.items():
            if at_h == h:
                @pl.when(c == at_c)
                def _(todo=todo):
                    for f, *n in todo:
                        f(*n)
                        if f is gA and n[0] + 1 < N:
                            gS(n[0] + 1)

    def st_out(tau):
        i = lax.rem(tau, TILES)
        return pltpu.make_async_copy(stb.at[i], ST.at[tau], st_sem.at[i])

    def pt_out(c, i):
        cols = tile(i)
        return pltpu.make_async_copy(pt.at[:, :, cols], PT.at[c, :, :, cols], pt_sem.at[i])

    def gate_up(slot, r, n):
        a = a_nat[r, :]
        g, u = dot(a, w_cols(slot, G_, n)), dot(a, w_cols(slot, U_, n))
        sig = jax.nn.sigmoid(g)
        silu = g * sig
        return silu, u * (sig + silu * (1.0 - sig)), (silu * u).astype(BF)

    def put_pt(p, i, n):
        nb = NH // BW
        pt[n * nb:(n + 1) * nb, :, tile(i, TM // SUB)] = p.T.reshape(nb, BW, TM // SUB)

    def fwd(c, carry):
        slot = lax.rem(c, 2)
        pl.when(c >= 2)(lambda: wait_weights(slot, 0))
        fwd_hook(0, c)

        def up_tile(i, _):
            pl.when(i == 1)(lambda: fwd_hook(1, c))

            @pl.when(c >= 1)
            def stored():
                st_out(TILES * (c - 1) + i).wait()
                pt_out(c - 1, i).wait()

            with jax.named_scope("fwd_up"):
                for j in range(SUB):
                    e = SUB * i + j
                    r = tile(e, TM // SUB)
                    inner = pl.ds(j * (TM // SUB), TM // SUB)
                    for n in range(CW // NH):
                        cols = pl.ds(n * NH, NH)
                        silu, slope, p = gate_up(slot, r, n)
                        stb[i, 0, inner, cols] = silu
                        stb[i, 1, inner, cols] = slope
                        put_pt(p, e, n)
                        dgu[0, r, cols] = p
            st_out(TILES * c + i).start()
            pt_out(c, i).start()
            return _

        lax.fori_loop(0, TILES, up_tile, 0)
        fwd_hook(2, c)
        pl.when(c >= 2)(lambda: wait_weights(slot, 1))

        @pl.when(c < C - 1)
        def _():
            with jax.named_scope("fwd_down"):
                for h in range(2):
                    acc[:, h * DH:(h + 1) * DH] += dot(dgu[0], wd_half(slot, h))

        @pl.when(c == C - 1)
        def _():
            a0t_out.wait()

            def one(j, _):
                with jax.named_scope("fwd_last"):
                    for e in range(NT // 4):
                        r = tile(NT // 4 * j + e, TN)
                        total = acc[r, :] + jnp.concatenate([dot(dgu[0, r, :], wd_half(slot, h)) for h in range(2)], axis=1)
                        h = (both(dyv, r).astype(F32) + total.astype(BF).astype(F32)).astype(BF)
                        for g in range(2):
                            dgu[g, r, :] = h[:, g * DH:(g + 1) * DH]
                        put_a(h.astype(F32), r)
                        acc[r, :] = jnp.zeros((TN, D), F32)
                r = tile(j, T // 4)
                for g in range(2):
                    pltpu.make_async_copy(dgu.at[g, r], H1.at[g, r], ld_sem.at[2]).start()
                for c_ in halves(dy_ref.at[0], dyv, r, ld_sem.at[0]):
                    c_.start()
                return _

            lax.fori_loop(0, 4, one, 0)

        fwd_hook(3, c)
        return carry

    lax.fori_loop(0, C, fwd, 0)
    for i in range(TILES):
        st_out(TILES * (C - 1) + i).wait()
        pt_out(C - 1, i).wait()
    pltpu.make_async_copy(dgu, H1, ld_sem.at[2]).wait()
    pltpu.make_async_copy(dyv, dyv, ld_sem.at[0]).wait()

    def d_p(slot, r, n):
        blocks = lambda h: wbuf[slot, D_, pl.ds(h * nx + n * (NH // BW), NH // BW)].reshape(NH, DH)
        return dot(dyv[0, r, :], blocks(0), 1, 1) + dot(dyv[1, r, :], blocks(1), 1, 1)

    def put_d(r, n, dp, silu, slope):
        cols = pl.ds(n * NH, NH)
        dgu[G_, r, cols] = (dp * slope).astype(BF)
        dgu[U_, r, cols] = (dp * silu).astype(BF)

    h1_in = [pltpu.make_async_copy(H1.at[h], a_nat.at[:, pl.ds(h * DH, DH)], ld_sem.at[0]) for h in range(2)]
    a0t_in = pltpu.make_async_copy(A0T, a_t, ld_sem.at[1])
    x_in = pltpu.make_async_copy(x_ref.at[0], a_nat, ld_sem.at[2])

    def st_load(c):
        for i in range(TILES):
            for e in range(2):
                pltpu.make_async_copy(ST.at[TILES * c + i, e], stb.at[i, e], st_sem.at[i]).start()

    def st_wait(i):
        pltpu.make_async_copy(stb.at[i], stb.at[i], st_sem.at[i]).wait()

    def pt_in(c):
        return pltpu.make_async_copy(PT.at[c], pt, pt_sem.at[0])

    def norm_back(h, d, through):
        scale = lax.rsqrt(jnp.mean(h * h, -1, keepdims=True) + 1e-6)
        along = jnp.sum(d * h, -1, keepdims=True) * (scale * scale * scale) * (1.0 / D)
        return (through + (d * scale - h * along)).astype(BF)

    def mid_tile(r):
        out = norm_back(a_nat[r, :].astype(F32), acc[r, :], both(dyv, r).astype(F32))
        for e in range(2):
            dyv[e, r, :] = out[:, e * DH:(e + 1) * DH]
        acc[r, :] = jnp.zeros((TN, D), F32)

    def middle():
        pltpu.make_async_copy(a_nat, a_nat, ld_sem.at[0]).wait()

        def mid(i, _):
            with jax.named_scope("mid"):
                mid_tile(tile(i, TN))
            return _

        lax.fori_loop(0, NT, mid, 0)
        x_in.start()
        a0t_in.wait()

    at_hook = {
        0: {0: [(gD, 2), (gA, 4), (gS, 5)], 1: [(gD, 4), (gB, 5), (gC, 5), (gE, 3), (gA, 6)], 2: [(gB, 6), (gC, 6)], 3: [(gE, 6)]},
        2: {0: [(gB, 3), (gC, 3), (gE, 2), (gB, 4), (gC, 4), (gA, 5), (gS, 6)], 1: [(gE, 4)], 2: [(gE, 5)]},
        3: {},
        4: {0: [(gD, 3)], 1: [(gD, 5)], 2: [(gD, 6)]},
    }

    def hook(h, m):
        for step, todo in at_hook[h].items():
            @pl.when(m == step)
            def _(todo=todo):
                for f, n in todo:
                    f(C + n)

    def dg_out(c):
        return pltpu.make_async_copy(dgu.at[:, pl.ds(T // 2, T // 2)], DGU.at[c], dg_sem.at[0])

    def d_a(slot, to, base):
        with jax.named_scope("da_tile"):
            r = pl.ds(base, T // 2)
            for h in range(2):
                acc[to:to + T // 2, h * DH:(h + 1) * DH] += (
                    dot(dgu[G_, r, :], w_half(slot, G_, h), 1, 1) + dot(dgu[U_, r, :], w_half(slot, U_, h), 1, 1))

    def bwd(m, carry):
        slot = lax.rem(m + 1, 2)
        last = m == C - 1
        first_layer = m >= C
        pl.when(m == C)(middle)
        wait_weights(slot, 1)

        @pl.when(first_layer & (m < 2 * C - 1))
        def _():
            load(m + 1 - C, 1 - slot, range(CORES), 0, 1)

        hook(0, m)

        @pl.when(jnp.logical_not(first_layer))
        def _():
            wait_weights(slot, 0)

            with jax.named_scope("bwd1_tile"):
                for e in range(TILES * SUB):
                    r = tile(e, TM // SUB)
                    for n in range(CW // NH):
                        silu, slope, p = gate_up(slot, r, n)
                        put_pt(p, e, n)
                        put_d(r, n, d_p(slot, r, n), silu, slope)

        @pl.when(first_layer)
        def _():
            pl.when(m > C)(lambda: dg_out(m - 1 - C).wait())
            for i in range(TILES):
                st_wait(i)
            with jax.named_scope("bwd0_tile"):
                for e in range(TILES * SUB):
                    r = pl.ds(e * (TM // SUB), TM // SUB)
                    inner = pl.ds((e % SUB) * (TM // SUB), TM // SUB)
                    for n in range(CW // NH):
                        cols = pl.ds(n * NH, NH)
                        put_d(r, n, d_p(slot, r, n), stb[e // SUB, 0, inner, cols], stb[e // SUB, 1, inner, cols])
            pl.when(m < 2 * C - 1)(lambda: dg_out(m - C).start())
            pt_in(m - C).wait()

        hook(2, m)
        lagged(x3, m - 2)

        @pl.when(last)
        def _():
            for c_ in h1_in:
                c_.start()
            load(0, 0, range(CORES), 0, 1)

        @pl.when((m >= C - 1) & (m < 2 * C - 1))
        def _():
            st_load(m + 1 - C)

        send_lanes(m)
        hook(3, m)

        @pl.when(m < C - 1)
        def _():
            gL(C + 1 + m)
            gF(C + 1 + m)

        pl.when(first_layer)(lambda: wait_weights(slot, 0))
        d_a(slot, 0, 0)
        lagged(x2, m - 1)
        hook(4, m)
        keep_lanes(m)
        x1(m)
        lagged(y2, m - 2)
        when(m >= 3, lambda: y3_out(m - 3))
        pl.when((m >= C - 1) & (m < 2 * C - 1))(lambda: pt_in(m + 1 - C).start())
        pl.when(last)(a0t_in.start)
        pl.when(m < C)(lambda: d_a(slot, T // 2, T // 2))
        return carry

    lax.fori_loop(0, 2 * C, bwd, 0)

    M = 2 * C

    def dg_in(c, half):
        return pltpu.make_async_copy(DGU.at[c], dgu.at[:, pl.ds(half * (T // 2), T // 2)], dg_sem.at[half])

    def late(j, carry):
        slot, half = lax.rem(j, 2), 1 - lax.rem(j, 2)

        @pl.when(j >= 1)
        def _():
            wait_weights(slot, 0)
            dg_in(j - 1, half).wait()

        @pl.when(j < C - 1)
        def _():
            load(j, 1 - slot, range(CORES), 0)
            dg_in(j, 1 - half).start()

        d_a(slot, T // 2, pl.multiple_of(half * (T // 2), T // 2))
        pl.when(j == 0)(lambda: x3(M - 2))
        pl.when(j == C - 6)(lambda: x2(M - 1))
        pl.when(j == C - 4)(lambda: y2(M - 2))
        pl.when(j == C - 3)(lambda: x3(M - 1))
        pl.when(j == C - 2)(lambda: y3(M - 3))
        return carry

    lax.fori_loop(0, C, late, 0)

    x_in.wait()

    def by_out(i):
        r = tile(i, TN)
        return pltpu.make_async_copy(a_nat.at[r], by_x.at[0, r], ld_sem.at[0])

    def last_norm(i, _):
        r = tile(i, TN)
        a_nat[r, :] = norm_back(a_nat[r, :].astype(F32), acc[r, :], both(dyv, r).astype(F32))
        by_out(i).start()
        return _

    lax.fori_loop(0, NT // 2, last_norm, 0)
    y2(M - 1)
    lax.fori_loop(NT // 2, NT, last_norm, 0)
    y3(M - 2)

    arrived(s_send, rs_send.at[0])
    arrived(two_, rs_send.at[1])
    arrived(one, rs_send.at[2])
    for layer in range(2):
        exchange(layer).wait_send()
    for n in range(N - 4, N):
        left_own(n)
        left_passed(n)
    pltpu.make_async_copy(a_nat, by_x.at[0], ld_sem.at[0]).wait()
    y3(M - 1)
    out_done(M - 1)
    arrived(od.at[:, :, pl.ds(0, DH)], od_recv)


def solution(mesh):
    nx, ny = mesh.shape["s"] // CORES, mesh.shape["r"]

    def step(x, dy, w_gate, w_up, w_down):
        layers, dr, ff = w_gate.shape
        _, T, D = x.shape
        C = ff // (nx * BW)
        N, CW, DH, HR = layers * C, nx * BW, D // 2, dr // 2
        TM = T // TILES

        hbm = pl.BlockSpec(memory_space=pltpu.HBM)
        shape = jax.ShapeDtypeStruct
        outs = pl.pallas_call(
            functools.partial(kernel, (nx, ny, C, T, D)),
            out_shape=[
                shape((1, T, D), BF), shape(w_gate.shape, BF), shape(w_up.shape, BF), shape(w_down.shape, BF),
                shape((N, 3, CORES * nx, dr, CW), BF), shape((layers, C * BW, DH), BF),
                shape((TILES * C, 2, TM, CW), F32), shape((C, nx, BW, T), BF),
                shape((nx, CORES, dr, T), BF), shape((2, T, DH), BF), shape((C, 2, T // 2, CW), BF),
            ],
            in_specs=[hbm] * 5,
            out_specs=[hbm] * 11,
            scratch_shapes=[
                pltpu.VMEM((T, D), BF), pltpu.VMEM((nx, CORES, dr, T), BF), pltpu.VMEM((2, T, DH), BF), pltpu.VMEM((T, D), F32),
                pltpu.VMEM((2, 3, CORES * nx, dr, CW), BF), pltpu.VMEM((2, T, CW), BF), pltpu.VMEM((nx, BW, T), BF),
                pltpu.VMEM((TILES, 2, TM, CW), F32), pltpu.VMEM((4, 3, dr, CW), BF),
                pltpu.VMEM((3, nx, dr, CW), BF), pltpu.VMEM((2, 3, nx, dr, CW), BF), pltpu.VMEM((2, 3, dr, CW), F32),
                pltpu.VMEM((3, HR, CW), F32), pltpu.VMEM((3, HR, CW), F32), pltpu.VMEM((3, dr, CW), BF),
                pltpu.VMEM((3, HR, CW), BF), pltpu.VMEM((3, HR, CW), BF), pltpu.VMEM((3, HR, CW), BF), pltpu.VMEM((3, HR, CW), BF),
                pltpu.VMEM((2, 3, HR, CW), BF), pltpu.VMEM((2, 3, HR, CW), BF),
                pltpu.VMEM((3, 3, dr, CW), BF), pltpu.VMEM((3, 3, dr, CW), BF), pltpu.VMEM((3, 3, dr, CW), BF),
                pltpu.VMEM((3, 3, dr, CW), BF), pltpu.VMEM((3, 3, dr, CW), BF), pltpu.VMEM((3, 3, dr, CW), BF),
                pltpu.VMEM((3, dr, CW), BF),
                *(pltpu.SemaphoreType.DMA(n) for n in (
                    (4, 2), (9, 5), (2, 2), (2,), (TILES,), (3,), (3,), (2,), (2,), (3,), (3,), (3, 2), (4,), (2,), (), (4,), (4,), (2,), (2,), (2,))),
            ],
            compiler_params=pltpu.CompilerParams(collective_id=0, has_side_effects=True, vmem_limit_bytes=67043328),
            name="stack",
        )(x, dy, w_gate, w_up, w_down)
        return tuple(outs[:4])

    states, cut = P(("rep", "r", "s"), None, None), P(None, "s", None)
    return jax.shard_map(
        step,
        mesh=mesh,
        in_specs=(states, states) + (cut,) * 3,
        out_specs=(states,) + (P("rep", "s", None),) * 3,
        check_vma=False,
    )
```

```python
import functools

import jax
import jax.numpy as jnp
from jax import lax
from jax.experimental import pallas as pl
from jax.experimental.pallas import tpu as pltpu
from jax.sharding import PartitionSpec as P

BF, F32 = jnp.bfloat16, jnp.float32
MESH = pl.DeviceIdType.MESH
CORES = 2
BW = 128
TILES = 2
NH = 256
SUB = 4
G_, U_, D_ = 0, 1, 2


def dot(a, b, ca=1, cb=0):
    return lax.dot_general(a, b, (((ca,), (cb,)), ((), ())), preferred_element_type=F32)


def when(condition, f):
    if isinstance(condition, bool):
        if condition:
            f()
    else:
        pl.when(condition)(f)


def kernel(dims, x_ref, dy_ref, wg_ref, wu_ref, wd_ref,
           by_x, og, ou, od, G, WDO, ST, PT, A0T, H1, DGU,
           a_nat, a_t, dyv, acc, wbuf, dgu, pt, stb, own_v,
           s_send, d_recv, own32, r32, l32, s_u1, s_pr, s_pl, u2r, u2l, ra, rb, rc, rd, v, ya, yb, yc, f_out,
           g_send, g_recv, w_sem, st_sem, pt_sem, ld_sem, rs_send, d_sem, x_sem, rc_sem, ys_sem, yr_sem, o_sem, od_send, od_recv,
           own_sem, own_out, ex_send, ex_recv, dg_sem):
    nx, ny, C, T, D = dims
    TM = T // TILES
    N = 2 * C
    DR = D // (CORES * nx)
    HR, QR = DR // 2, DR // 4
    CW = nx * BW
    DH = D // 2

    s, y = lax.axis_index("s"), lax.axis_index("r")
    X, k = lax.div(s, CORES), lax.rem(s, CORES)
    at = lambda xx, kk: CORES * lax.rem(xx, nx) + kk
    right, left = {"s": at(X + 1, k)}, {"s": at(X + nx - 1, k)}
    sib = {"s": at(X, 1 - k)}
    up, down = {"r": lax.rem(y + 1, ny)}, {"r": lax.rem(y + ny - 1, ny)}

    def remote(src, dst, ss, rs, who):
        return pltpu.make_async_remote_copy(src_ref=src, dst_ref=dst, send_sem=ss, recv_sem=rs, device_id=who, device_id_type=MESH)

    def arrived(dst, rs):
        pltpu.make_async_copy(dst, dst, rs).wait()

    packet = lambda xx: k * nx + lax.rem(xx, nx)
    own, pL, pR, pO = packet(X), packet(X + nx - 1), packet(X + 1), packet(X + 2)
    par = lax.rem(y, 2)
    mine, other = par * HR, (1 - par) * HR

    def rows(base, q):
        return pl.ds(pl.multiple_of(base + q * QR, QR), QR)

    PARTS = {None: pl.ds(0, 3), 0: pl.ds(0, 2), 1: pl.ds(2, 1)}

    def home(n):
        return wbuf.at[n] if n < 2 else G.at[n]

    def kept(n):
        return pltpu.make_async_copy(wbuf.at[n], G.at[n], w_sem.at[n, 0])

    def out_copy(t, n, part=None):
        full = pl.ds(0, DR)
        spec = {
            0: (None, rows(mine, 0), right), 1: (None, rows(mine, 1), right),
            2: (None, rows(mine, 1), left), 3: (None, rows(mine, 0), left),
            4: (pL, rows(mine, 0), right), 5: (pR, rows(mine, 1), left),
            6: (pL, rows(mine, 0), up), 7: (pR, rows(mine, 0), up), 8: (pO, rows(mine, 0), up),
            9: (pL, rows(mine, 1), down), 10: (pR, rows(mine, 1), down), 11: (pO, rows(mine, 1), down),
            12: (None, full, sib), 13: (pL, full, sib), 14: (pR, full, sib), 15: (pO, full, sib),
        }
        j, r, who = spec[t]
        q = PARTS[part]
        src = own_v.at[lax.rem(n, 4), q, r, :] if j is None else home(n).at[q, j, r, :]
        dst = home(n).at[q, own if j is None else j, r, :]
        leaves = g_send.at[lax.rem(n, 4), 0 if j is None else 1]
        return remote(src, dst, leaves, g_recv.at[8 if part == 1 else lax.rem(n, 8), STAGE[t]], who)

    STAGE = (0, 1, 0, 1, 2, 2, 3, 3, 3, 3, 3, 3, 4, 4, 4, 4)

    def in_wait(i, n, part=None):
        q = PARTS[part]
        to = (G.at[n, q, 0, pl.ds(0, HR)],) * 3 + (G.at[n, q, pl.ds(0, 3), pl.ds(0, HR)], G.at[n, q, pl.ds(0, 4)])
        arrived(to[i], g_recv.at[8 if part == 1 else lax.rem(n, 8), i])

    def left_own(n):
        arrived(G.at[n, :, pl.ds(0, 2)], g_send.at[lax.rem(n, 4), 0])

    def left_passed(n):
        arrived(G.at[n, :, pl.ds(0, 5)], g_send.at[lax.rem(n, 4), 1])

    def named(f):
        def run(*args):
            with jax.named_scope(f.__name__):
                return f(*args)
        return run

    def stage(f):
        return lambda n, *part: when((n >= 0) & (n < N) if not isinstance(n, int) else 0 <= n < N, lambda: named(f)(n, *part))

    def starts(n, part, *ts):
        for t in ts:
            out_copy(t, n, part).start()

    def layer_of(n):
        if isinstance(n, int):
            return n // C, n % C
        second = n >= C
        return jnp.where(second, 1, 0), jnp.where(second, n - C, n)

    def block_cols(j, c):
        return pl.ds(pl.multiple_of((j * C + c) * BW, BW), BW)

    def half_block(h):
        o = jnp.where(h >= C, 1, 0)
        return o, pl.ds(pl.multiple_of(HR * (h - C * o), HR), HR)

    def core_cols(core):
        return pl.ds(pl.multiple_of(core * DH, DH), DH)

    def exchange(layer):
        mine_ = pl.ds(pl.multiple_of(k * C * HR, HR), C * HR)
        return remote(wd_ref.at[layer, :, core_cols(1 - k)], WDO.at[layer, mine_], ex_send.at[layer], ex_recv.at[layer], sib)

    def exchanged(layer):
        theirs = pl.ds(pl.multiple_of((1 - k) * C * HR, HR), C * HR)
        arrived(WDO.at[layer, theirs], ex_recv.at[layer])

    def own_down(n, sem):
        slot, (layer, c) = lax.rem(n, 4), layer_of(n)
        for e in range(2):
            h = 2 * c + e
            o, r = half_block(h)
            dst = own_v.at[slot, D_, pl.ds(e * HR, HR)]
            far = pl.ds(pl.multiple_of(HR * h, HR), HR)
            pl.when(o == k)(lambda: pltpu.make_async_copy(wd_ref.at[layer, r, core_cols(k)], dst, sem).start())
            pl.when(o != k)(lambda: pltpu.make_async_copy(WDO.at[layer, far], dst, sem).start())

    def own_cols(n):
        slot, (layer, c) = lax.rem(n, 4), layer_of(n)
        for q, w in ((G_, wg_ref), (U_, wu_ref)):
            for j in range(nx):
                pltpu.make_async_copy(w.at[layer, :, block_cols(j, c)], own_v.at[slot, q, :, pl.ds(j * BW, BW)], own_sem.at[slot]).start()

    @stage
    def gS(n):
        when(n >= 4, lambda: left_own(n - 4))
        own_cols(n)
        own_down(n, own_sem.at[lax.rem(n, 4)])

    def own_stored(n):
        return pltpu.make_async_copy(own_v.at[lax.rem(n, 4)], home(n).at[:, own], own_out.at[lax.rem(n, 4)])

    @stage
    def gA(n):
        slot = lax.rem(n, 4)
        pltpu.make_async_copy(own_v.at[slot], own_v.at[slot], own_sem.at[slot]).wait()
        starts(n, None, 0, 2, 1, 3, 12)
        own_stored(n).start()

    @stage
    def gB(n, part=None):
        when(n >= 6, lambda: left_passed(n - 4))
        in_wait(0, n, part)
        starts(n, part, 4, 5, 6, 10)

    @stage
    def gC(n, part=None):
        in_wait(1, n, part)
        starts(n, part, 9, 7)

    @stage
    def gD(n, part=None):
        in_wait(2, n, part)
        starts(n, part, 8, 11)

    @stage
    def gE(n, part=None):
        in_wait(3, n, part)
        starts(n, part, 13, 14, 15)
        if part != 1:
            own_stored(n).wait()

    def lane(core):
        return pl.ds(pl.multiple_of(core * nx, nx), nx)

    def load(n, slot, lanes, *parts):
        for part in parts:
            for core in lanes:
                at_ = (PARTS[part], lane(core))
                pltpu.make_async_copy(G.at[n, *at_], wbuf.at[slot, *at_], w_sem.at[slot, part]).start()

    def wait_weights(slot, part):
        to = wbuf.at[slot, PARTS[part]]
        pltpu.make_async_copy(to, to, w_sem.at[slot, part]).wait()

    @stage
    def gL(n):
        if isinstance(n, int) and n in (2, 3):
            left_passed(n - 2)
            kept(n - 2).wait()
        load(n, lax.rem(n, 2), (k,), 0, 1)

    @stage
    def gF(n, part=None):
        in_wait(4, n, part)
        if isinstance(n, int) and n < 2:
            if part != 0:
                kept(n).start()
        else:
            load(n, lax.rem(n, 2), (1 - k,), 0, 1)

    def w_cols(slot, q, n):
        cols = pl.ds(n * NH, NH)
        return jnp.concatenate([wbuf[slot, q, c * nx + x, :, cols] for x in range(nx) for c in range(CORES)], axis=0)

    def w_half(slot, q, h):
        return jnp.concatenate([wbuf[slot, q, c * nx + h * (nx // 2) + x] for x in range(nx // 2) for c in range(CORES)], axis=0)

    def wd_half(slot, h):
        return wbuf[slot, D_, pl.ds(h * nx, nx)].reshape(CW, DH)

    def tile(i, n=None):
        n = TM if n is None else n
        return pl.ds(pl.multiple_of(i * n, n), n)

    def rel(j):
        return lax.rem(X + j, nx)

    def lane_lhs(lane):
        return jnp.concatenate([a_t[rel(j), lane] for j in range(nx)], axis=0)

    def grad(q, lane):
        if q == D_:
            lhs = jnp.concatenate([pt[rel(j)] for j in range(nx)], axis=0)
            return dot(lhs, dyv[lane])
        return dot(lane_lhs(lane), dgu[q])

    def d_copy(q, m):
        return remote(s_send.at[q], d_recv.at[lax.rem(m, 2), q], rs_send.at[0], d_sem.at[lax.rem(m, 2)], sib)

    def send_lane(q, m):
        s_send[q] = grad(q, 1 - k).astype(BF).reshape(nx, DR, CW)

    @named
    def send_lanes(m):
        when(m > 0, lambda: arrived(s_send, rs_send.at[0]))
        send_lane(D_, m)
        send_lane(G_, m)
        d_copy(D_, m).start()
        d_copy(G_, m).start()
        send_lane(U_, m)
        d_copy(U_, m).start()

    lo, hi = pl.ds(0, HR), pl.ds(HR, HR)

    one, two_ = v.at[0], v.at[pl.ds(0, 2)]

    def x_copy(t, m):
        two, three = lax.rem(m, 2), lax.rem(m, 3)
        src, dst, sem, who = {
            0: (s_u1.at[:, lo], ra.at[two], x_sem.at[two], right),
            1: (s_u1.at[:, hi], rb.at[two], x_sem.at[two], left),
            2: (s_pr, rc.at[three, :, hi], rc_sem.at[three], right),
            3: (s_pl, rd.at[three, :, lo], rc_sem.at[three], left),
            4: (u2r, rc.at[three, :, lo], rc_sem.at[three], right),
            5: (u2l, rd.at[three, :, hi], rc_sem.at[three], left),
        }[t]
        return remote(src, dst, rs_send.at[1 if t < 4 else 2], sem, who)

    turn = jnp.where(par == 0, 1, ny - 1)
    first_pair, second_pair = {"r": lax.rem(y + turn, ny)}, {"r": lax.rem(y + ny - turn, ny)}

    def y_copy(t, m):
        three = lax.rem(m, 3)
        src, dst, who = {
            0: (v.at[three, :, lo], ya.at[three, :, lo], first_pair),
            1: (v.at[three, :, hi], ya.at[three, :, hi], second_pair),
            2: (yb.at[three, :, lo], yc.at[three, :, lo], second_pair),
            3: (yb.at[three, :, hi], yc.at[three, :, hi], first_pair),
        }[t]
        return remote(src, dst, ys_sem.at[three], yr_sem.at[three, t // 2], who)

    @named
    def keep_lanes(m):
        two = lax.rem(m, 2)

        when(m > 0, lambda: arrived(two_, rs_send.at[1]))
        when(m >= 3, lambda: y3_wait(m - 3))
        arrived(d_recv.at[two], d_sem.at[two])
        for q in (D_, G_, U_):
            if q == G_:
                y3_add(m - 3)
            total = (grad(q, k) + d_recv[two, q].reshape(CW, CW).astype(F32)).reshape(nx, DR, CW)
            own32[two, q] = total[0]
            r32[q] = total[1, :HR]
            s_pr[q] = total[1, HR:].astype(BF)
            s_u1[q] = total[2].astype(BF)
            s_pl[q] = total[3, :HR].astype(BF)
            l32[q] = total[3, HR:]

    @named
    def x1(m):
        for t in range(4):
            x_copy(t, m).start()

    def slot_of(m, n):
        return lax.rem(m + n, n)

    @named
    def x2_wait(m):
        arrived(one, x_sem.at[lax.rem(m, 2)])
        when(m > 0, lambda: arrived(one, rs_send.at[2]))

    def x2_add(m):
        two = slot_of(m, 2)
        for q in range(3):
            u2r[q] = (r32[q] + ra[two, q].astype(F32)).astype(BF)
            u2l[q] = (l32[q] + rb[two, q].astype(F32)).astype(BF)

    def x2_out(m):
        x_copy(4, m).start()
        x_copy(5, m).start()

    def x2(m):
        x2_wait(m)
        x2_add(m)
        x2_out(m)

    @named
    def x3(m):
        arrived(two_, rc_sem.at[lax.rem(m, 3)])
        two, three = lax.rem(m, 2), lax.rem(m, 3)
        for q in range(3):
            v[three, q] = (own32[two, q] + rc[three, q].astype(F32) + rd[three, q].astype(F32)).astype(BF)
        for t in (0, 1):
            y_copy(t, m).start()

    @named
    def y2(m):
        three = lax.rem(m, 3)
        arrived(one, yr_sem.at[three, 0])
        for q in range(3):
            yb[three, q] = (v[three, q].astype(F32) + ya[three, q].astype(F32)).astype(BF)
        for t in (2, 3):
            y_copy(t, m).start()

    def where_m(m):
        first = m < C
        return jnp.where(first, 1, 0), jnp.where(first, m, m - C)

    def cols_out(q, m):
        layer, c = where_m(m)
        return [pltpu.make_async_copy(f_out.at[q, :, pl.ds(j * BW, BW)], (og, ou)[q].at[layer, :, block_cols(j, c)], o_sem.at[q])
                for j in range(nx)]

    def od_each(m, local, far):
        layer, c = where_m(m)
        for e in range(2):
            o, r = half_block(2 * c + e)
            src, dst = f_out.at[D_, pl.ds(e * HR, HR)], od.at[layer, r, core_cols(k)]
            pl.when(o == k)(functools.partial(local, pltpu.make_async_copy(src, dst, o_sem.at[2 + e])))
            pl.when(o != k)(functools.partial(far, remote(src, dst, od_send.at[e], od_recv, sib)))

    @named
    def out_done(m):
        for q in (G_, U_):
            pltpu.make_async_copy(f_out.at[q], f_out.at[q], o_sem.at[q]).wait()
        od_each(m, lambda c: c.wait(), lambda c: c.wait_send())

    @named
    def y3_wait(m):
        arrived(one, yr_sem.at[lax.rem(m, 3), 1])
        when(m > 0, lambda: out_done(m - 1))

    def y3_add(m):
        three = slot_of(m, 3)
        for q in range(3):
            f_out[q] = (yb[three, q].astype(F32) + yc[three, q].astype(F32)).astype(BF)

    @named
    def y3_out(m):
        arrived(two_, ys_sem.at[lax.rem(m, 3)])
        for q in (G_, U_):
            for c_ in cols_out(q, m):
                c_.start()
        od_each(m, lambda c: c.start(), lambda c: c.start())

    def y3(m):
        y3_wait(m)
        y3_add(m)
        y3_out(m)

    def lagged(f, m):
        when(m >= 0, lambda: f(m))

    def halves(src, dst, r, sem):
        return [pltpu.make_async_copy(src.at[r, pl.ds(h * DH, DH)], dst.at[h, r], sem) for h in range(2)]

    every = pl.ds(0, T)
    own_cols(0)
    for c_ in halves(x_ref.at[0], dyv, every, ld_sem.at[0]):
        c_.start()

    barrier = pltpu.get_barrier_semaphore()
    for who in (right, left, sib, up, down):
        pl.semaphore_signal(barrier, inc=1, device_id=who, device_id_type=MESH)
    with jax.named_scope("entry"):
        pl.semaphore_wait(barrier, 5)

    for layer in range(2):
        exchange(layer).start()
    first = own_v.at[0, PARTS[0]]
    with jax.named_scope("own_wait"):
        pltpu.make_async_copy(first, first, own_sem.at[0]).wait()
    starts(0, 0, 0, 2, 1, 3, 12)
    own_cols(1)
    named(exchanged)(0)
    own_down(0, ld_sem.at[2])
    own_down(1, own_sem.at[1])
    pltpu.make_async_copy(dyv, dyv, ld_sem.at[0]).wait()

    NT = 4 * TILES
    TN = T // NT

    def both(ref, r):
        return jnp.concatenate([ref[0, r, :], ref[1, r, :]], axis=1)

    def put_a(h, r):
        scale = lax.rsqrt(jnp.mean(h * h, -1, keepdims=True) + 1e-6)
        a = (h * scale).astype(BF)
        a_nat[r, :] = a
        a_t[:, :, :, r] = a.T.reshape(nx, CORES, DR, TN)

    def norm0(i, _):
        r = tile(i, TN)
        put_a(both(dyv, r).astype(F32), r)
        acc[r, :] = jnp.zeros((TN, D), F32)
        return _

    lax.fori_loop(0, NT // 4, norm0, 0)
    first = own_v.at[0, PARTS[1]]
    pltpu.make_async_copy(first, first, ld_sem.at[2]).wait()
    starts(0, 1, 0, 2, 1, 3, 12)
    own_stored(0).start()
    lax.fori_loop(NT // 4, NT, norm0, 0)
    a0t_out = pltpu.make_async_copy(a_t, A0T, ld_sem.at[1])
    a0t_out.start()
    gB(0, 0)
    gC(0, 0)
    gB(0, 1)
    gA(1)
    gC(0, 1)
    exchanged(1)
    gS(2)
    gD(0, 0)
    gD(0, 1)
    gB(1)
    gA(2)
    gS(3)
    gE(0, 0)
    gE(0, 1)
    gF(0, 0)

    A, B, C_, D__, E, F, L = gA, gB, gC, gD, gE, gF, gL
    fwd_hooks = {
        (0, 0): [(C_, 1), (F, 0, 1)], (0, 1): [(D__, 1), (B, 2), (A, 3)], (0, 2): [(C_, 2), (E, 1)], (0, 3): [(D__, 2), (F, 1)],
        (1, 0): [(B, 3), (A, 4)], (1, 1): [(C_, 3), (E, 2), (L, 2)], (1, 2): [(D__, 3), (B, 4), (F, 2), (A, 5)], (1, 3): [(C_, 4)],
        (2, 1): [(E, 3), (L, 3), (D__, 4)], (2, 2): [(B, 5), (C_, 5), (F, 3), (A, 6)], (2, 3): [(E, 4)],
        (3, 0): [(L, 4)], (3, 1): [(D__, 5)], (3, 2): [(F, 4), (B, 6), (C_, 6), (A, 7)], (3, 3): [(E, 5)],
        (4, 0): [(L, 5)], (4, 1): [(D__, 6)], (4, 2): [(F, 5), (B, 7), (A, 8)], (4, 3): [(C_, 7), (E, 6)],
        (5, 0): [(L, 6)], (5, 1): [(D__, 7)], (5, 2): [(F, 6), (B, 8), (A, 9)], (5, 3): [(C_, 8), (E, 7)],
        (6, 0): [(L, 7)], (6, 1): [(D__, 8)], (6, 2): [(F, 7), (B, 9), (A, 10)], (6, 3): [(C_, 9), (E, 8)],
    }

    def fwd_hook(h, c):
        for (at_c, at_h), todo in fwd_hooks.items():
            if at_h == h:
                @pl.when(c == at_c)
                def _(todo=todo):
                    for f, *n in todo:
                        f(*n)
                        if f is gA and n[0] + 1 < N:
                            gS(n[0] + 1)

    def st_out(tau):
        i = lax.rem(tau, TILES)
        return pltpu.make_async_copy(stb.at[i], ST.at[tau], st_sem.at[i])

    def pt_out(c, i):
        cols = tile(i)
        return pltpu.make_async_copy(pt.at[:, :, cols], PT.at[c, :, :, cols], pt_sem.at[i])

    def gate_up(slot, r, n):
        a = a_nat[r, :]
        g, u = dot(a, w_cols(slot, G_, n)), dot(a, w_cols(slot, U_, n))
        sig = jax.nn.sigmoid(g)
        silu = g * sig
        return silu, u * (sig + silu * (1.0 - sig)), (silu * u).astype(BF)

    def put_pt(p, i, n):
        nb = NH // BW
        pt[n * nb:(n + 1) * nb, :, tile(i, TM // SUB)] = p.T.reshape(nb, BW, TM // SUB)

    def fwd(c, carry):
        slot = lax.rem(c, 2)
        pl.when(c >= 2)(lambda: wait_weights(slot, 0))
        fwd_hook(0, c)

        def up_tile(i, _):
            pl.when(i == 1)(lambda: fwd_hook(1, c))

            @pl.when(c >= 1)
            def stored():
                st_out(TILES * (c - 1) + i).wait()
                pt_out(c - 1, i).wait()

            with jax.named_scope("fwd_up"):
                for j in range(SUB):
                    e = SUB * i + j
                    r = tile(e, TM // SUB)
                    inner = pl.ds(j * (TM // SUB), TM // SUB)
                    for n in range(CW // NH):
                        cols = pl.ds(n * NH, NH)
                        silu, slope, p = gate_up(slot, r, n)
                        stb[i, 0, inner, cols] = silu
                        stb[i, 1, inner, cols] = slope
                        put_pt(p, e, n)
                        dgu[0, r, cols] = p
            st_out(TILES * c + i).start()
            pt_out(c, i).start()
            return _

        lax.fori_loop(0, TILES, up_tile, 0)
        fwd_hook(2, c)
        pl.when(c >= 2)(lambda: wait_weights(slot, 1))

        @pl.when(c < C - 1)
        def _():
            with jax.named_scope("fwd_down"):
                for e in range(2):
                    r = pl.ds(e * (T // 2), T // 2)
                    for h in range(2):
                        acc[r, h * DH:(h + 1) * DH] += dot(dgu[0, r, :], wd_half(slot, h))

        @pl.when(c == C - 1)
        def _():
            a0t_out.wait()

            def one(j, _):
                with jax.named_scope("fwd_last"):
                    for e in range(NT // 4):
                        r = tile(NT // 4 * j + e, TN)
                        total = acc[r, :] + jnp.concatenate([dot(dgu[0, r, :], wd_half(slot, h)) for h in range(2)], axis=1)
                        h = (both(dyv, r).astype(F32) + total.astype(BF).astype(F32)).astype(BF)
                        for g in range(2):
                            dgu[g, r, :] = h[:, g * DH:(g + 1) * DH]
                        put_a(h.astype(F32), r)
                        acc[r, :] = jnp.zeros((TN, D), F32)
                r = tile(j, T // 4)
                for g in range(2):
                    pltpu.make_async_copy(dgu.at[g, r], H1.at[g, r], ld_sem.at[2]).start()
                for c_ in halves(dy_ref.at[0], dyv, r, ld_sem.at[0]):
                    c_.start()
                return _

            lax.fori_loop(0, 4, one, 0)

        fwd_hook(3, c)
        return carry

    lax.fori_loop(0, C, fwd, 0)
    for i in range(TILES):
        st_out(TILES * (C - 1) + i).wait()
        pt_out(C - 1, i).wait()
    pltpu.make_async_copy(dgu, H1, ld_sem.at[2]).wait()
    pltpu.make_async_copy(dyv, dyv, ld_sem.at[0]).wait()

    def d_p(slot, r, n):
        blocks = lambda h: wbuf[slot, D_, pl.ds(h * nx + n * (NH // BW), NH // BW)].reshape(NH, DH)
        return dot(dyv[0, r, :], blocks(0), 1, 1) + dot(dyv[1, r, :], blocks(1), 1, 1)

    def put_d(r, n, dp, silu, slope):
        cols = pl.ds(n * NH, NH)
        dgu[G_, r, cols] = (dp * slope).astype(BF)
        dgu[U_, r, cols] = (dp * silu).astype(BF)

    h1_in = [pltpu.make_async_copy(H1.at[h], a_nat.at[:, pl.ds(h * DH, DH)], ld_sem.at[0]) for h in range(2)]
    a0t_in = pltpu.make_async_copy(A0T, a_t, ld_sem.at[1])
    x_in = pltpu.make_async_copy(x_ref.at[0], a_nat, ld_sem.at[2])

    def st_load(c):
        for i in range(TILES):
            for e in range(2):
                pltpu.make_async_copy(ST.at[TILES * c + i, e], stb.at[i, e], st_sem.at[i]).start()

    def st_wait(i):
        pltpu.make_async_copy(stb.at[i], stb.at[i], st_sem.at[i]).wait()

    def pt_in(c):
        return pltpu.make_async_copy(PT.at[c], pt, pt_sem.at[0])

    def norm_back(h, d, through):
        scale = lax.rsqrt(jnp.mean(h * h, -1, keepdims=True) + 1e-6)
        along = jnp.sum(d * h, -1, keepdims=True) * (scale * scale * scale) * (1.0 / D)
        return (through + (d * scale - h * along)).astype(BF)

    def mid_tile(r):
        out = norm_back(a_nat[r, :].astype(F32), acc[r, :], both(dyv, r).astype(F32))
        for e in range(2):
            dyv[e, r, :] = out[:, e * DH:(e + 1) * DH]
        acc[r, :] = jnp.zeros((TN, D), F32)

    def middle():
        pltpu.make_async_copy(a_nat, a_nat, ld_sem.at[0]).wait()

        def mid(i, _):
            with jax.named_scope("mid"):
                mid_tile(tile(i, TN))
            return _

        lax.fori_loop(0, NT, mid, 0)
        x_in.start()
        a0t_in.wait()

    at_hook = {
        0: {0: [(gD, 2), (gA, 4), (gS, 5)], 1: [(gD, 4), (gB, 5), (gC, 5), (gE, 3), (gA, 6)], 2: [(gB, 6), (gC, 6)]},
        2: {0: [(gB, 3), (gC, 3), (gE, 2), (gB, 4), (gC, 4), (gA, 5), (gS, 6)], 1: [(gE, 4)], 2: [(gE, 5)], 3: [(gE, 6)]},
        3: {},
        4: {0: [(gD, 3)], 1: [(gD, 5)], 2: [(gD, 6)]},
    }

    def hook(h, m):
        for step, todo in at_hook[h].items():
            @pl.when(m == step)
            def _(todo=todo):
                for f, n in todo:
                    f(C + n)

    def dg_out(c):
        return pltpu.make_async_copy(dgu.at[:, pl.ds(T // 2, T // 2)], DGU.at[c], dg_sem.at[0])

    def d_a(slot, to, base):
        with jax.named_scope("da_tile"):
            r = pl.ds(base, T // 2)
            for h in range(2):
                acc[to:to + T // 2, h * DH:(h + 1) * DH] += (
                    dot(dgu[G_, r, :], w_half(slot, G_, h), 1, 1) + dot(dgu[U_, r, :], w_half(slot, U_, h), 1, 1))

    def bwd(m, carry):
        slot = lax.rem(m + 1, 2)
        last = m == C - 1
        first_layer = m >= C
        pl.when(m == C)(middle)
        wait_weights(slot, 1)

        @pl.when(first_layer & (m < 2 * C - 1))
        def _():
            load(m + 1 - C, 1 - slot, range(CORES), 0, 1)

        hook(0, m)

        @pl.when(jnp.logical_not(first_layer))
        def _():
            wait_weights(slot, 0)

            with jax.named_scope("bwd1_tile"):
                for e in range(TILES * SUB):
                    r = tile(e, TM // SUB)
                    for n in range(CW // NH):
                        silu, slope, p = gate_up(slot, r, n)
                        put_pt(p, e, n)
                        put_d(r, n, d_p(slot, r, n), silu, slope)

        @pl.when(first_layer)
        def _():
            pl.when(m > C)(lambda: dg_out(m - 1 - C).wait())
            for i in range(TILES):
                st_wait(i)
            with jax.named_scope("bwd0_tile"):
                for e in range(TILES * SUB):
                    r = pl.ds(e * (TM // SUB), TM // SUB)
                    inner = pl.ds((e % SUB) * (TM // SUB), TM // SUB)
                    for n in range(CW // NH):
                        cols = pl.ds(n * NH, NH)
                        put_d(r, n, d_p(slot, r, n), stb[e // SUB, 0, inner, cols], stb[e // SUB, 1, inner, cols])
            pl.when(m < 2 * C - 1)(lambda: dg_out(m - C).start())
            pt_in(m - C).wait()

        hook(2, m)
        lagged(x3, m - 2)

        @pl.when(last)
        def _():
            for c_ in h1_in:
                c_.start()
            load(0, 0, range(CORES), 0, 1)

        @pl.when((m >= C - 1) & (m < 2 * C - 1))
        def _():
            st_load(m + 1 - C)

        send_lanes(m)
        hook(3, m)

        @pl.when(m < C - 1)
        def _():
            gL(C + 1 + m)
            gF(C + 1 + m)

        pl.when(first_layer)(lambda: wait_weights(slot, 0))
        d_a(slot, 0, 0)
        lagged(x2, m - 1)
        hook(4, m)
        keep_lanes(m)
        x1(m)
        lagged(y2, m - 2)
        when(m >= 3, lambda: y3_out(m - 3))
        pl.when((m >= C - 1) & (m < 2 * C - 1))(lambda: pt_in(m + 1 - C).start())
        pl.when(last)(a0t_in.start)
        pl.when(m < C)(lambda: d_a(slot, T // 2, T // 2))
        return carry

    lax.fori_loop(0, 2 * C, bwd, 0)

    M = 2 * C

    def dg_in(c, half):
        return pltpu.make_async_copy(DGU.at[c], dgu.at[:, pl.ds(half * (T // 2), T // 2)], dg_sem.at[half])

    def late(j, carry):
        slot, half = lax.rem(j, 2), 1 - lax.rem(j, 2)

        @pl.when(j >= 1)
        def _():
            wait_weights(slot, 0)
            dg_in(j - 1, half).wait()

        @pl.when(j < C - 1)
        def _():
            load(j, 1 - slot, range(CORES), 0)
            dg_in(j, 1 - half).start()

        d_a(slot, T // 2, pl.multiple_of(half * (T // 2), T // 2))
        pl.when(j == 0)(lambda: x3(M - 2))
        pl.when(j == C - 6)(lambda: x2(M - 1))
        pl.when(j == C - 4)(lambda: y2(M - 2))
        pl.when(j == C - 3)(lambda: x3(M - 1))
        pl.when(j == C - 2)(lambda: y3(M - 3))
        return carry

    lax.fori_loop(0, C, late, 0)

    x_in.wait()

    def by_out(i):
        r = tile(i, TN)
        return pltpu.make_async_copy(a_nat.at[r], by_x.at[0, r], ld_sem.at[0])

    def last_norm(i, _):
        r = tile(i, TN)
        a_nat[r, :] = norm_back(a_nat[r, :].astype(F32), acc[r, :], both(dyv, r).astype(F32))
        by_out(i).start()
        return _

    lax.fori_loop(0, NT // 2, last_norm, 0)
    y2(M - 1)
    lax.fori_loop(NT // 2, NT, last_norm, 0)
    y3(M - 2)

    arrived(s_send, rs_send.at[0])
    arrived(two_, rs_send.at[1])
    arrived(one, rs_send.at[2])
    for layer in range(2):
        exchange(layer).wait_send()
    for n in range(N - 4, N):
        left_own(n)
        left_passed(n)
    pltpu.make_async_copy(a_nat, by_x.at[0], ld_sem.at[0]).wait()
    y3(M - 1)
    out_done(M - 1)
    arrived(od.at[:, :, pl.ds(0, DH)], od_recv)


def solution(mesh):
    nx, ny = mesh.shape["s"] // CORES, mesh.shape["r"]

    def step(x, dy, w_gate, w_up, w_down):
        layers, dr, ff = w_gate.shape
        _, T, D = x.shape
        C = ff // (nx * BW)
        N, CW, DH, HR = layers * C, nx * BW, D // 2, dr // 2
        TM = T // TILES

        hbm = pl.BlockSpec(memory_space=pltpu.HBM)
        shape = jax.ShapeDtypeStruct
        outs = pl.pallas_call(
            functools.partial(kernel, (nx, ny, C, T, D)),
            out_shape=[
                shape((1, T, D), BF), shape(w_gate.shape, BF), shape(w_up.shape, BF), shape(w_down.shape, BF),
                shape((N, 3, CORES * nx, dr, CW), BF), shape((layers, C * BW, DH), BF),
                shape((TILES * C, 2, TM, CW), F32), shape((C, nx, BW, T), BF),
                shape((nx, CORES, dr, T), BF), shape((2, T, DH), BF), shape((C, 2, T // 2, CW), BF),
            ],
            in_specs=[hbm] * 5,
            out_specs=[hbm] * 11,
            scratch_shapes=[
                pltpu.VMEM((T, D), BF), pltpu.VMEM((nx, CORES, dr, T), BF), pltpu.VMEM((2, T, DH), BF), pltpu.VMEM((T, D), F32),
                pltpu.VMEM((2, 3, CORES * nx, dr, CW), BF), pltpu.VMEM((2, T, CW), BF), pltpu.VMEM((nx, BW, T), BF),
                pltpu.VMEM((TILES, 2, TM, CW), F32), pltpu.VMEM((4, 3, dr, CW), BF),
                pltpu.VMEM((3, nx, dr, CW), BF), pltpu.VMEM((2, 3, nx, dr, CW), BF), pltpu.VMEM((2, 3, dr, CW), F32),
                pltpu.VMEM((3, HR, CW), F32), pltpu.VMEM((3, HR, CW), F32), pltpu.VMEM((3, dr, CW), BF),
                pltpu.VMEM((3, HR, CW), BF), pltpu.VMEM((3, HR, CW), BF), pltpu.VMEM((3, HR, CW), BF), pltpu.VMEM((3, HR, CW), BF),
                pltpu.VMEM((2, 3, HR, CW), BF), pltpu.VMEM((2, 3, HR, CW), BF),
                pltpu.VMEM((3, 3, dr, CW), BF), pltpu.VMEM((3, 3, dr, CW), BF), pltpu.VMEM((3, 3, dr, CW), BF),
                pltpu.VMEM((3, 3, dr, CW), BF), pltpu.VMEM((3, 3, dr, CW), BF), pltpu.VMEM((3, 3, dr, CW), BF),
                pltpu.VMEM((3, dr, CW), BF),
                *(pltpu.SemaphoreType.DMA(n) for n in (
                    (4, 2), (9, 5), (2, 2), (2,), (TILES,), (3,), (3,), (2,), (2,), (3,), (3,), (3, 2), (4,), (2,), (), (4,), (4,), (2,), (2,), (2,))),
            ],
            compiler_params=pltpu.CompilerParams(collective_id=0, has_side_effects=True, vmem_limit_bytes=67043328),
            name="stack",
        )(x, dy, w_gate, w_up, w_down)
        return tuple(outs[:4])

    states, cut = P(("rep", "r", "s"), None, None), P(None, "s", None)
    return jax.shard_map(
        step,
        mesh=mesh,
        in_specs=(states, states) + (cut,) * 3,
        out_specs=(states,) + (P("rep", "s", None),) * 3,
        check_vma=False,
    )
```
